16 devices in a mesh: rep: 2 (over y, z), g: 8 (over x, core).
Axes of the slice: x: 4, y: 2, z: 1, core: 2. Of those that a mesh axis runs over, the one named last changes fastest.
The devices are a block of a 4x4x8 slice.
Arguments:
- hidden: bfloat16 [512, 6144], P(('rep', 'g')), parts along dimension 0
- cache_lat: bfloat16 [512, 1024, 512], P(('rep', 'g')), parts along dimension 0
- cache_rope: bfloat16 [512, 1024, 64], P(('rep', 'g')), parts along dimension 0
- seq_lens: int32 [512], P(('rep', 'g')), parts along dimension 0
- gain_attn: bfloat16 [6144], replicated
- w_dq: bfloat16 [6144, 1536], replicated
- gain_q: bfloat16 [1536], replicated
- w_uq: bfloat16 [1536, 64, 128], replicated
- w_qr: bfloat16 [1536, 64, 64], replicated
- w_dkv: bfloat16 [6144, 576], replicated
- gain_kv: bfloat16 [512], replicated
- w_uk: bfloat16 [512, 64, 128], replicated
- w_uv: bfloat16 [512, 64, 128], replicated
- w_o: bfloat16 [8192, 6144], replicated
- gain_mlp: bfloat16 [6144], replicated
- w_gate: bfloat16 [6144, 12288], P(None, 'g')
- w_up: bfloat16 [6144, 12288], P(None, 'g')
- w_down: bfloat16 [12288, 6144], P('g')
Outputs:
- output 1: bfloat16 [512, 6144], P(('rep', 'g')), parts along dimension 0
- output 2: bfloat16 [512, 512], P(('rep', 'g')), parts along dimension 0
- output 3: bfloat16 [512, 64], P(('rep', 'g')), parts along dimension 0
There are 2 independent parts. The reference program is written for one: setup_inputs(seed, part) draws one part's arguments, and reference() takes and returns one part's arrays. A program takes and returns all parts, laid end to end along the dimension named above; an argument that names none is the same for every part.
All inputs are finite; a program needn't handle non-finite values.
Results may differ from the reference program's by a relative error of at most 0.0123806.
Values are sent between devices in bfloat16 or wider.
A program may use at most 768 MiB of HBM per device.

```python
import jax
import jax.numpy as jnp
from jax import lax

BATCH_ROWS = 256
CACHE_LEN = 1024
D_MODEL = 6144
NUM_HEADS = 64
Q_LORA = 1536
KV_LORA = 512
ROPE_DIM = 64
NOPE_DIM = 128
V_DIM = 128
FFN_DIM = 12288


def rms_norm(values, gain_vec):
    mean_sq = jnp.mean(jnp.square(values), axis=-1, keepdims=True)
    return values * lax.rsqrt(mean_sq + 1e-6) * gain_vec.astype(jnp.float32)


def apply_rope(values, positions):
    half_dim = values.shape[-1] // 2
    inv_freq = 10000.0 ** (-jnp.arange(half_dim).astype(jnp.float32) / half_dim)
    angles = positions.astype(jnp.float32)[..., None] * inv_freq
    cos_part = jnp.cos(angles)
    sin_part = jnp.sin(angles)
    first_half = values[..., :half_dim]
    second_half = values[..., half_dim:]
    return jnp.concatenate([first_half * cos_part - second_half * sin_part, first_half * sin_part + second_half * cos_part], axis=-1)


def draw_normal(rand_key, arr_shape, spread):
    return (jax.random.normal(rand_key, arr_shape, jnp.float32) * spread).astype(jnp.bfloat16)


def draw_gain(rand_key, length):
    return jax.random.uniform(rand_key, (length,), jnp.float32, 0.5, 1.5).astype(jnp.bfloat16)


def draw_lens(rand_key):
    len_key, pick_key = jax.random.split(rand_key)
    lens_drawn = jax.random.randint(len_key, (BATCH_ROWS,), CACHE_LEN // 4, CACHE_LEN + 1, dtype=jnp.int32)
    pick_order = jax.random.permutation(pick_key, BATCH_ROWS)
    return lens_drawn.at[pick_order[0]].set(CACHE_LEN).at[pick_order[1]].set(CACHE_LEN // 4)


def setup_inputs(seed: int = 0, part: int = 0) -> dict:
    row_keys = jax.random.split(jax.random.fold_in(jax.random.key(seed), part), 4)
    weight_keys = jax.random.split(jax.random.key(seed + 1), 14)
    return {
        "hidden": draw_normal(row_keys[0], (BATCH_ROWS, D_MODEL), 1.0),
        "cache_lat": draw_normal(row_keys[1], (BATCH_ROWS, CACHE_LEN, KV_LORA), 1.0),
        "cache_rope": draw_normal(row_keys[2], (BATCH_ROWS, CACHE_LEN, ROPE_DIM), 1.0),
        "seq_lens": draw_lens(row_keys[3]),
        "gain_attn": draw_gain(weight_keys[0], D_MODEL),
        "w_dq": draw_normal(weight_keys[1], (D_MODEL, Q_LORA), D_MODEL ** -0.5),
        "gain_q": draw_gain(weight_keys[2], Q_LORA),
        "w_uq": draw_normal(weight_keys[3], (Q_LORA, NUM_HEADS, NOPE_DIM), Q_LORA ** -0.5),
        "w_qr": draw_normal(weight_keys[4], (Q_LORA, NUM_HEADS, ROPE_DIM), Q_LORA ** -0.5),
        "w_dkv": draw_normal(weight_keys[5], (D_MODEL, KV_LORA + ROPE_DIM), D_MODEL ** -0.5),
        "gain_kv": draw_gain(weight_keys[6], KV_LORA),
        "w_uk": draw_normal(weight_keys[7], (KV_LORA, NUM_HEADS, NOPE_DIM), (3 * NOPE_DIM) ** -0.5),
        "w_uv": draw_normal(weight_keys[8], (KV_LORA, NUM_HEADS, V_DIM), KV_LORA ** -0.5 * CACHE_LEN ** 0.5 / 4),
        "w_o": draw_normal(weight_keys[9], (NUM_HEADS * V_DIM, D_MODEL), (NUM_HEADS * V_DIM) ** -0.5),
        "gain_mlp": draw_gain(weight_keys[10], D_MODEL),
        "w_gate": draw_normal(weight_keys[11], (D_MODEL, FFN_DIM), D_MODEL ** -0.5),
        "w_up": draw_normal(weight_keys[12], (D_MODEL, FFN_DIM), D_MODEL ** -0.5),
        "w_down": draw_normal(weight_keys[13], (FFN_DIM, D_MODEL), FFN_DIM ** -0.5),
    }


def reference(hidden, cache_lat, cache_rope, seq_lens, gain_attn, w_dq, gain_q, w_uq, w_qr, w_dkv, gain_kv, w_uk, w_uv, w_o, gain_mlp, w_gate, w_up, w_down):
    normed = rms_norm(hidden.astype(jnp.float32), gain_attn).astype(jnp.bfloat16)
    q_in = rms_norm(jnp.dot(normed, w_dq, preferred_element_type=jnp.float32), gain_q).astype(jnp.bfloat16)
    q_nope = jnp.einsum("bq,qhn->bhn", q_in.astype(jnp.float32), w_uq.astype(jnp.float32)).astype(jnp.bfloat16)
    q_rope = apply_rope(jnp.einsum("bq,qhr->bhr", q_in.astype(jnp.float32), w_qr.astype(jnp.float32)), seq_lens[:, None]).astype(jnp.bfloat16)
    kv_raw = jnp.dot(normed, w_dkv, preferred_element_type=jnp.float32)
    new_lat = rms_norm(kv_raw[:, :KV_LORA], gain_kv).astype(jnp.bfloat16)
    new_rope = apply_rope(kv_raw[:, KV_LORA:], seq_lens).astype(jnp.bfloat16)
    q_abs = jnp.einsum("bhn,chn->bhc", q_nope.astype(jnp.float32), w_uk.astype(jnp.float32)).astype(jnp.bfloat16)
    score_scale = (NOPE_DIM + ROPE_DIM) ** -0.5
    key_pos = jnp.arange(CACHE_LEN)

    def one_row(row_data):
        q_lat, q_rot, lat_rows, rope_rows, row_len, lat_new, rope_new = row_data
        past_score = (jnp.einsum("hc,lc->hl", q_lat.astype(jnp.float32), lat_rows.astype(jnp.float32)) + jnp.einsum("hr,lr->hl", q_rot.astype(jnp.float32), rope_rows.astype(jnp.float32))) * score_scale
        own_score = (jnp.einsum("hc,c->h", q_lat.astype(jnp.float32), lat_new.astype(jnp.float32)) + jnp.einsum("hr,r->h", q_rot.astype(jnp.float32), rope_new.astype(jnp.float32))) * score_scale
        past_score = jnp.where(key_pos[None, :] < row_len, past_score, -jnp.inf)
        row_max = jnp.maximum(jnp.max(past_score, axis=-1), own_score)
        past_exp = jnp.exp(past_score - row_max[:, None])
        own_exp = jnp.exp(own_score - row_max)
        row_total = jnp.sum(past_exp, axis=-1) + own_exp
        past_prob = (past_exp / row_total[:, None]).astype(jnp.bfloat16)
        own_prob = (own_exp / row_total).astype(jnp.bfloat16)
        mixed_lat = jnp.einsum("hl,lc->hc", past_prob.astype(jnp.float32), lat_rows.astype(jnp.float32)) + own_prob.astype(jnp.float32)[:, None] * lat_new.astype(jnp.float32)[None, :]
        return mixed_lat.astype(jnp.bfloat16)

    out_lat = lax.map(one_row, (q_abs, q_rope, cache_lat, cache_rope, seq_lens, new_lat, new_rope))
    out_heads = jnp.einsum("bhc,chv->bhv", out_lat.astype(jnp.float32), w_uv.astype(jnp.float32)).astype(jnp.bfloat16)
    attn_out = jnp.dot(out_heads.reshape(BATCH_ROWS, NUM_HEADS * V_DIM), w_o, preferred_element_type=jnp.float32)
    resid_rows = (hidden.astype(jnp.float32) + attn_out).astype(jnp.bfloat16)
    mlp_in = rms_norm(resid_rows.astype(jnp.float32), gain_mlp).astype(jnp.bfloat16)
    gate_proj = jnp.dot(mlp_in, w_gate, preferred_element_type=jnp.float32)
    up_proj = jnp.dot(mlp_in, w_up, preferred_element_type=jnp.float32)
    act_vals = (jax.nn.silu(gate_proj) * up_proj).astype(jnp.bfloat16)
    out_hidden = (resid_rows.astype(jnp.float32) + jnp.dot(act_vals, w_down, preferred_element_type=jnp.float32)).astype(jnp.bfloat16)
    return out_hidden, new_lat, new_rope
```

```python
import functools

import jax
import jax.numpy as jnp
from jax import lax
from jax.experimental import pallas as pl
from jax.experimental.pallas import tpu as pltpu
from jax.sharding import PartitionSpec as P


def rms_norm(values, gain_vec):
    mean_sq = jnp.mean(jnp.square(values), axis=-1, keepdims=True)
    return values * lax.rsqrt(mean_sq + 1e-6) * gain_vec.astype(jnp.float32)


def apply_rope(values, positions):
    half_dim = values.shape[-1] // 2
    inv_freq = 10000.0 ** (-jnp.arange(half_dim).astype(jnp.float32) / half_dim)
    angles = positions.astype(jnp.float32)[..., None] * inv_freq
    cos_part = jnp.cos(angles)
    sin_part = jnp.sin(angles)
    first_half = values[..., :half_dim]
    second_half = values[..., half_dim:]
    return jnp.concatenate([first_half * cos_part - second_half * sin_part, first_half * sin_part + second_half * cos_part], axis=-1)


ATT_BLK = 256
ATT_BUF = 4
UV_HEADS = 16


def attn_kernel(lens_ref, q_ref, qr_ref, nl_ref, nr_ref, nl_rows, lat_hbm, rope_hbm, wuv_hbm, o_ref, lat_buf, rope_buf, mix, wuv, lat_sem, rope_sem, wuv_sem):
    rows, heads, kv_dim = q_ref.shape
    cache_len = lat_hbm.shape[1]
    scale = (wuv.shape[2] + qr_ref.shape[2]) ** -0.5
    max_blk = cache_len // ATT_BLK

    def lat_copy(row, blk, slot):
        span = pl.ds(blk * ATT_BLK, ATT_BLK)
        return pltpu.make_async_copy(lat_hbm.at[row, span], lat_buf.at[slot, span], lat_sem.at[slot, blk])

    def rope_copy(row, slot):
        return pltpu.make_async_copy(rope_hbm.at[row], rope_buf.at[slot], rope_sem.at[slot])

    def blocks(row):
        return (lens_ref[row] + ATT_BLK - 1) // ATT_BLK

    def fetch(row, slot):
        count = blocks(row)
        rope_copy(row, slot).start()
        for blk in range(max_blk):
            @pl.when(blk < count)
            def _():
                lat_copy(row, blk, slot).start()

    for row in range(ATT_BUF - 1):
        fetch(row, row)
    wuv_copy = pltpu.make_async_copy(wuv_hbm, wuv, wuv_sem)
    wuv_copy.start()

    own_col = lax.broadcasted_iota(jnp.int32, (heads, rows), 1)
    nl_all = nl_ref[...]
    nr_all = nr_ref[...]
    nt = (((1,), (1,)), ((), ()))

    def one_row(row, carry):
        slot = lax.rem(row, ATT_BUF)
        ahead = row + ATT_BUF - 1

        @pl.when(ahead < rows)
        def _():
            fetch(ahead, lax.rem(ahead, ATT_BUF))

        count = blocks(row)
        length = lens_ref[row]
        rope_copy(row, slot).wait()
        for blk in range(max_blk):
            @pl.when(blk < count)
            def _():
                lat_copy(row, blk, slot).wait()

        for num in range(1, max_blk + 1):
            @pl.when(count == num)
            def _():
                span = num * ATT_BLK
                lat = lat_buf[slot, :span]
                q_lat = q_ref[row]
                q_rot = qr_ref[row]
                s = lax.dot_general(q_lat, lat, nt, preferred_element_type=jnp.float32)
                s = s + jnp.dot(q_rot, rope_buf[slot, :, :span], preferred_element_type=jnp.float32)
                s = s * scale
                own = lax.dot_general(q_lat, nl_all, nt, preferred_element_type=jnp.float32) + lax.dot_general(q_rot, nr_all, nt, preferred_element_type=jnp.float32)
                own = jnp.sum(jnp.where(own_col == row, own, 0.0), axis=1, keepdims=True) * scale
                pos = lax.broadcasted_iota(jnp.int32, (heads, span), 1)
                s = jnp.where(pos < length, s, -jnp.inf)
                top = jnp.maximum(jnp.max(s, axis=1, keepdims=True), own)
                e = jnp.exp(s - top)
                own_e = jnp.exp(own - top)
                inv = 1.0 / (jnp.sum(e, axis=1, keepdims=True) + own_e)
                prob = (e * inv).astype(jnp.bfloat16)
                own_p = (own_e * inv).astype(jnp.bfloat16).astype(jnp.float32)
                acc = jnp.dot(prob, lat, preferred_element_type=jnp.float32)
                acc = acc + own_p * nl_rows[row].astype(jnp.float32)
                mix[row] = acc.astype(jnp.bfloat16)
        return carry

    lax.fori_loop(0, rows, one_row, 0)
    wuv_copy.wait()

    def head_group(grp, carry):
        base = pl.multiple_of(grp * UV_HEADS, UV_HEADS)
        lhs = mix[:, pl.ds(base, UV_HEADS), :].reshape(rows, UV_HEADS * kv_dim)
        rhs = wuv[:, pl.ds(base, UV_HEADS), :].reshape(kv_dim, UV_HEADS * wuv.shape[2])
        v_dim = wuv.shape[2]
        for h in range(UV_HEADS):
            part = jnp.dot(lhs[:, h * kv_dim : (h + 1) * kv_dim], rhs[:, h * v_dim : (h + 1) * v_dim], preferred_element_type=jnp.float32)
            o_ref[:, pl.ds(pl.multiple_of(grp * UV_HEADS * v_dim, v_dim) + h * v_dim, v_dim)] = part.astype(jnp.bfloat16)
        return carry

    lax.fori_loop(0, heads // UV_HEADS, head_group, 0)


def attention(lens, q_abs, q_rope, new_lat, new_rope, cache_lat, rope_t, w_uv):
    rows, heads, kv_dim = q_abs.shape
    cache_len = cache_lat.shape[1]
    rope_dim = q_rope.shape[2]
    v_dim = w_uv.shape[2]
    vmem = pl.BlockSpec(memory_space=pltpu.VMEM)
    hbm = pl.BlockSpec(memory_space=pl.ANY)
    max_blk = cache_len // ATT_BLK
    return pl.pallas_call(
        attn_kernel,
        out_shape=jax.ShapeDtypeStruct((rows, heads * v_dim), jnp.bfloat16),
        in_specs=[pl.BlockSpec(memory_space=pltpu.SMEM), vmem, vmem, vmem, vmem, vmem, hbm, hbm, hbm],
        out_specs=vmem,
        scratch_shapes=[
            pltpu.VMEM((ATT_BUF, cache_len, kv_dim), jnp.bfloat16),
            pltpu.VMEM((ATT_BUF, rope_dim, cache_len), jnp.bfloat16),
            pltpu.VMEM((rows, heads, kv_dim), jnp.bfloat16),
            pltpu.VMEM((kv_dim, heads, v_dim), jnp.bfloat16),
            pltpu.SemaphoreType.DMA((ATT_BUF, max_blk)),
            pltpu.SemaphoreType.DMA((ATT_BUF,)),
            pltpu.SemaphoreType.DMA,
        ],
        compiler_params=pltpu.CompilerParams(vmem_limit_bytes=40 * 2**20),
        cost_estimate=pl.CostEstimate(flops=10**10, bytes_accessed=40 * 10**6, transcendentals=0),
        name="attention",
    )(lens, q_abs, q_rope, new_lat, new_rope, new_lat[:, None, :], cache_lat, rope_t, w_uv)


MESH = pl.DeviceIdType.MESH
RING = 14
TILE_K = 2048
TILE_N = 512
SEND_N = 256


def mlp_kernel(n_dev, o_ref, x_ref, gain_ref, wo_hbm, wg_hbm, wu_hbm, wd_hbm, out_ref,
               ring, o_all, x_all, h_all, m_all, u_own, u_peer, wd_peer, acc, part, own_part, near, relay, far, fin,
               ring_sem, pair_sem, gat_send, gat_recv, u_sem, rs_send, rs_recv):
    rows, d_model = x_ref.shape
    heads_dim = o_ref.shape[1]
    half = d_model // 2
    ff = wg_hbm.shape[1]
    chips = n_dev // 2
    pair = 2 * rows
    total = n_dev * rows
    f32 = jnp.float32
    me = lax.axis_index("g")
    core = me % 2
    chip = me // 2
    peer = chip * 2 + (1 - core)
    right_chip = (chip + 1) % chips
    left_chip = (chip + chips - 1) % chips
    far_chip = (chip + 2) % chips
    right = right_chip * 2 + core
    left = left_chip * 2 + core
    col0 = pl.multiple_of(core * half, half)
    other0 = pl.multiple_of((1 - core) * half, half)

    def remote(src, dst, send, recv, dev):
        return pltpu.make_async_remote_copy(src_ref=src, dst_ref=dst, send_sem=send, recv_sem=recv, device_id={"g": dev}, device_id_type=MESH)

    wo_k = heads_dim // TILE_K
    sub = SEND_N * wo_k
    wo_j = half // TILE_N
    n_wo = wo_j * wo_k
    gu_k = d_model // TILE_K
    gu_n = ff // TILE_N
    n_gu = gu_n * 2 * gu_k
    wd_n = half // TILE_N
    n_all = n_wo + n_gu + wd_n

    def ring_copy(src, slot, depth):
        return pltpu.make_async_copy(src, ring.at[slot, pl.ds(0, depth)], ring_sem.at[slot])

    def issue(t):
        slot = t % RING

        @pl.when(t < n_wo)
        def _():
            j, k = t // wo_k, t % wo_k
            ring_copy(wo_hbm.at[pl.ds(pl.multiple_of(k * TILE_K, TILE_K), TILE_K), pl.ds(pl.multiple_of(col0 + j * TILE_N, TILE_N), TILE_N)], slot, TILE_K).start()

        for mat, w_hbm in ((0, wg_hbm), (1, wu_hbm)):
            q = t - n_wo

            @pl.when((q >= 0) & (q < n_gu) & ((q // gu_k) % 2 == mat))
            def _():
                n, k = q // (2 * gu_k), q % gu_k
                ring_copy(w_hbm.at[pl.ds(pl.multiple_of(k * TILE_K, TILE_K), TILE_K), pl.ds(pl.multiple_of(n * TILE_N, TILE_N), TILE_N)], slot, TILE_K).start()

        @pl.when((t >= n_wo + n_gu) & (t < n_all))
        def _():
            n = t - n_wo - n_gu
            ring_copy(wd_hbm.at[:, pl.ds(pl.multiple_of(col0 + n * TILE_N, TILE_N), TILE_N)], slot, ff).start()

    def arrive(t, depth):
        slot = t % RING
        ring_copy(wo_hbm.at[pl.ds(0, depth), pl.ds(0, TILE_N)], slot, depth).wait()
        return slot

    for t in range(RING):
        issue(jnp.int32(t))

    barrier = pltpu.get_barrier_semaphore()
    for dev in (peer, left, right):
        pl.semaphore_signal(barrier, inc=1, device_id={"g": dev}, device_id_type=MESH)
    pl.semaphore_wait(barrier, 3)

    my_rows = pl.ds(pl.multiple_of(core * rows, rows), rows)
    peer_rows = pl.ds(pl.multiple_of((1 - core) * rows, rows), rows)
    o_copy = remote(o_ref, o_all.at[my_rows], pair_sem.at[0], pair_sem.at[1], peer)
    x_copy = remote(x_ref.at[:, pl.ds(other0, half)], x_all.at[my_rows], pair_sem.at[2], pair_sem.at[3], peer)
    wd_copy = remote(wd_hbm.at[:, pl.ds(other0, half)], wd_peer, pair_sem.at[4], pair_sem.at[5], peer)
    o_copy.start()
    x_copy.start()
    wd_copy.start()
    o_all[my_rows, :] = o_ref[...]
    x_all[my_rows, :] = x_ref[:, pl.ds(col0, half)]
    o_copy.wait()
    x_copy.wait()

    def rows_of(c, lo, num):
        return pl.ds(pl.multiple_of(c * pair + lo, rows), num)

    def chunk_cols(s):
        return pl.ds(pl.multiple_of(col0 + s * SEND_N, SEND_N), SEND_N)

    def near_copy(s, to_right):
        region = h_all.at[rows_of(chip, 0, pair), chunk_cols(s)]
        side = 0 if to_right else 1
        return remote(region, region, gat_send.at[side, s], gat_recv.at[side, s], right if to_right else left)

    def pass_copy(s, to_right):
        src_chip = left_chip if to_right else right_chip
        region = h_all.at[rows_of(src_chip, 0 if to_right else rows, rows), chunk_cols(s)]
        side = 2 if to_right else 3
        return remote(region, region, gat_send.at[side, s], gat_recv.at[side, s], right if to_right else left)

    def peer_copy(s):
        region = h_all.at[:, chunk_cols(s)]
        return remote(region, region, gat_send.at[4, s], gat_recv.at[4, s], peer)

    n_send = half // SEND_N
    per_step = TILE_N // SEND_N

    def gather_step(s):
        for back, act in ((0, 0), (3, 1), (6, 2)):
            c = s - back

            @pl.when((c >= 0) & (c < n_send))
            def _():
                if act == 0:
                    near_copy(c, True).start()
                    near_copy(c, False).start()
                elif act == 1:
                    near_copy(c, True).wait_recv()
                    near_copy(c, False).wait_recv()
                    pass_copy(c, True).start()
                    pass_copy(c, False).start()
                else:
                    pass_copy(c, True).wait_recv()
                    pass_copy(c, False).wait_recv()
                    peer_copy(c).start()

    def wo_step(j, carry):
        for k in range(wo_k):
            if k % (wo_k // per_step) == 0:
                gather_step(per_step * (j - 1) + k // (wo_k // per_step))
            slot = arrive(j * wo_k + k, TILE_K)
            prod = jnp.dot(o_all[:, k * TILE_K : (k + 1) * TILE_K], ring[slot], preferred_element_type=f32)
            if k == 0:
                acc[:pair] = prod
            elif k < wo_k - 1:
                acc[:pair] += prod
            else:
                xs = x_all[:, pl.ds(pl.multiple_of(j * TILE_N, TILE_N), TILE_N)].astype(f32)
                h_all[rows_of(chip, 0, pair), pl.ds(pl.multiple_of(col0 + j * TILE_N, TILE_N), TILE_N)] = (xs + (acc[:pair] + prod)).astype(jnp.bfloat16)
            issue(j * wo_k + k + RING)
        return carry

    lax.fori_loop(0, wo_j, wo_step, 0)

    def drain(s, carry):
        gather_step(s)
        return carry

    lax.fori_loop(per_step * (wo_j - 1), n_send + 6, drain, 0)

    def settle(s, carry):
        peer_copy(s).wait()
        for to_right in (True, False):
            near_copy(s, to_right).wait_send()
            pass_copy(s, to_right).wait_send()
        return carry

    lax.fori_loop(0, n_send, settle, 0)

    def norm_rows(b, carry):
        block = pl.ds(pl.multiple_of(b * 16, 16), 16)
        lanes = jnp.zeros((16, 128), f32)
        for c in range(0, d_model, 512):
            v = h_all[block, c : c + 512].astype(f32)
            sq = v * v
            lanes = lanes + ((sq[:, :128] + sq[:, 128:256]) + (sq[:, 256:384] + sq[:, 384:]))
        inv = lax.rsqrt(jnp.sum(lanes, axis=1, keepdims=True) / d_model + 1e-6)
        for c in range(0, d_model, 512):
            v = h_all[block, c : c + 512].astype(f32)
            m_all[block, c : c + 512] = (v * inv * gain_ref[:, c : c + 512].astype(f32)).astype(jnp.bfloat16)
        return carry

    lax.fori_loop(0, total // 16, norm_rows, 0)

    def u_copy(n):
        span = pl.ds(pl.multiple_of(n * TILE_N, TILE_N), TILE_N)
        return remote(u_own.at[:, span], u_peer.at[:, span], u_sem.at[0, n], u_sem.at[1, n], peer)

    def gu_step(n, carry):
        for mat in range(2):
            for k in range(gu_k):
                t = n_wo + n * 2 * gu_k + mat * gu_k + k
                slot = arrive(t, TILE_K)
                prod = jnp.dot(m_all[:, k * TILE_K : (k + 1) * TILE_K], ring[slot], preferred_element_type=f32)
                if k == 0:
                    acc[pl.ds(mat * total, total)] = prod
                else:
                    acc[pl.ds(mat * total, total)] += prod
                issue(t + RING)
        span = pl.ds(pl.multiple_of(n * TILE_N, TILE_N), TILE_N)
        for b in range(0, total, 64):
            g = acc[b : b + 64]
            u_own[b : b + 64, span] = (jax.nn.silu(g) * acc[total + b : total + b + 64]).astype(jnp.bfloat16)
        u_copy(n).start()
        return carry

    lax.fori_loop(0, gu_n, gu_step, 0)
    wd_copy.wait()
    for n in range(gu_n):
        u_copy(n).wait()

    def span_of(n):
        return pl.ds(pl.multiple_of(n * TILE_N, TILE_N), TILE_N)

    def rs_near(n, to_right):
        side = 0 if to_right else 1
        c = right_chip if to_right else left_chip
        return remote(part.at[rows_of(c, 0, pair), span_of(n)], near.at[side, :, span_of(n)], rs_send.at[side, n], rs_recv.at[side, n], right if to_right else left)

    def rs_far(n, to_right):
        side = 0 if to_right else 1
        return remote(part.at[rows_of(far_chip, side * rows, rows), span_of(n)], relay.at[side, :, span_of(n)], rs_send.at[2 + side, n], rs_recv.at[2 + side, n], right if to_right else left)

    def rs_pass(n, to_right):
        side = 0 if to_right else 1
        return remote(relay.at[side, :, span_of(n)], far.at[side, :, span_of(n)], rs_send.at[4 + side, n], rs_recv.at[4 + side, n], right if to_right else left)

    def out_cols(n):
        return pl.ds(pl.multiple_of(col0 + n * TILE_N, TILE_N), TILE_N)

    def rs_out(n):
        return remote(fin.at[:, span_of(n)], out_ref.at[:, out_cols(n)], rs_send.at[6, n], rs_recv.at[6, n], peer)

    def down_step(n, carry):
        t = n_wo + n_gu + n
        slot = arrive(t, ff)
        acc[:total] = jnp.dot(u_own[...], ring[slot, :ff], preferred_element_type=f32)
        acc[:total] += jnp.dot(u_peer[...], wd_peer[:, span_of(n)], preferred_element_type=f32)
        part[:, span_of(n)] = acc[:total].astype(jnp.bfloat16)
        own_part[:, span_of(n)] = acc[rows_of(chip, 0, pair), :]
        for to_right in (True, False):
            rs_far(n, to_right).start()
        for to_right in (True, False):
            rs_near(n, to_right).start()
        return carry

    lax.fori_loop(0, wd_n, down_step, 0)

    def final_step(s, carry):
        @pl.when(s < wd_n)
        def _():
            for to_right in (True, False):
                rs_far(s, to_right).wait_recv()
                rs_pass(s, to_right).start()

        @pl.when(s >= 1)
        def _():
            n = s - 1
            for to_right in (True, False):
                rs_near(n, to_right).wait_recv()
                rs_pass(n, to_right).wait_recv()
            span = span_of(n)

            def rows_sum(lo_static, lo):
                blk = pl.ds(pl.multiple_of(lo, rows), rows)
                mlp = own_part[blk, span] + near[0, blk, span].astype(f32) + near[1, blk, span].astype(f32) + far[lo_static, :, span].astype(f32)
                return (h_all[rows_of(chip, lo, rows), out_cols(n)].astype(f32) + mlp).astype(jnp.bfloat16)

            low = rows_sum(0, 0)
            high = rows_sum(1, rows)
            mine = jnp.where(core == 0, low, high)
            out_ref[:, out_cols(n)] = mine
            fin[:, span] = jnp.where(core == 0, high, low)
            rs_out(n).start()

        return carry

    lax.fori_loop(0, wd_n + 1, final_step, 0)

    def finish(n, carry):
        rs_out(n).wait()
        for to_right in (True, False):
            rs_near(n, to_right).wait_send()
            rs_far(n, to_right).wait_send()
            rs_pass(n, to_right).wait_send()
        return carry

    lax.fori_loop(0, wd_n, finish, 0)


def out_proj_mlp(n_dev, o, x, gain, w_o, w_gate, w_up, w_down):
    rows, d_model = x.shape
    half = d_model // 2
    ff = w_gate.shape[1]
    pair, total = 2 * rows, n_dev * rows
    bf16, f32 = jnp.bfloat16, jnp.float32
    vmem = pl.BlockSpec(memory_space=pltpu.VMEM)
    hbm = pl.BlockSpec(memory_space=pl.ANY)
    n_send, wd_n = half // SEND_N, half // TILE_N
    dma = pltpu.SemaphoreType.DMA
    return pl.pallas_call(
        functools.partial(mlp_kernel, n_dev),
        out_shape=jax.ShapeDtypeStruct((rows, d_model), bf16),
        in_specs=[vmem, vmem, vmem, hbm, hbm, hbm, hbm],
        out_specs=vmem,
        scratch_shapes=[
            pltpu.VMEM((RING, TILE_K, TILE_N), bf16),
            pltpu.VMEM((pair, o.shape[1]), bf16),
            pltpu.VMEM((pair, half), bf16),
            pltpu.VMEM((total, d_model), bf16),
            pltpu.VMEM((total, d_model), bf16),
            pltpu.VMEM((total, ff), bf16),
            pltpu.VMEM((total, ff), bf16),
            pltpu.VMEM((ff, half), bf16),
            pltpu.VMEM((2 * total, TILE_N), f32),
            pltpu.VMEM((total, half), bf16),
            pltpu.VMEM((pair, half), f32),
            pltpu.VMEM((2, pair, half), bf16),
            pltpu.VMEM((2, rows, half), bf16),
            pltpu.VMEM((2, rows, half), bf16),
            pltpu.VMEM((rows, half), bf16),
            dma((RING,)),
            dma((6,)),
            dma((5, n_send)),
            dma((5, n_send)),
            dma((2, ff // TILE_N)),
            dma((7, wd_n)),
            dma((7, wd_n)),
        ],
        compiler_params=pltpu.CompilerParams(vmem_limit_bytes=67043328, collective_id=1, has_side_effects=True),
        cost_estimate=pl.CostEstimate(flops=2 * 10**10, bytes_accessed=116 * 10**6, transcendentals=0),
        name="out_proj_mlp",
    )(o, x, gain, w_o, w_gate, w_up, w_down)


def attention_rows(hidden, cache_lat, cache_rope, seq_lens, gain_attn, w_dq, gain_q, w_uq, w_qr, w_dkv, gain_kv, w_uk, w_uv, w_o):
    kv_dim = w_uk.shape[0]
    normed = rms_norm(hidden.astype(jnp.float32), gain_attn).astype(jnp.bfloat16)
    q_in = rms_norm(jnp.dot(normed, w_dq, preferred_element_type=jnp.float32), gain_q).astype(jnp.bfloat16)
    q_nope = jnp.einsum("bq,qhn->bhn", q_in, w_uq, preferred_element_type=jnp.float32).astype(jnp.bfloat16)
    q_rope = apply_rope(jnp.einsum("bq,qhr->bhr", q_in, w_qr, preferred_element_type=jnp.float32), seq_lens[:, None]).astype(jnp.bfloat16)
    kv_raw = jnp.dot(normed, w_dkv, preferred_element_type=jnp.float32)
    new_lat = rms_norm(kv_raw[:, :kv_dim], gain_kv).astype(jnp.bfloat16)
    new_rope = apply_rope(kv_raw[:, kv_dim:], seq_lens).astype(jnp.bfloat16)
    q_abs = jnp.einsum("bhn,chn->bhc", q_nope, w_uk, preferred_element_type=jnp.float32).astype(jnp.bfloat16)
    out_heads = attention(seq_lens, q_abs, q_rope, new_lat, new_rope, cache_lat, jnp.swapaxes(cache_rope, 1, 2), w_uv)
    return out_heads, new_lat, new_rope


def solution(mesh):
    row_spec = P(("rep", "g"))
    full_spec = P()
    in_specs = (row_spec, row_spec, row_spec, row_spec, full_spec, full_spec, full_spec, full_spec, full_spec, full_spec, full_spec, full_spec, full_spec, full_spec, full_spec, P(None, "g"), P(None, "g"), P("g", None))

    def local_step(hidden, cache_lat, cache_rope, seq_lens, gain_attn, w_dq, gain_q, w_uq, w_qr, w_dkv, gain_kv, w_uk, w_uv, w_o, gain_mlp, w_gate, w_up, w_down):
        out_heads, new_lat, new_rope = attention_rows(hidden, cache_lat, cache_rope, seq_lens, gain_attn, w_dq, gain_q, w_uq, w_qr, w_dkv, gain_kv, w_uk, w_uv, w_o)
        out_hidden = out_proj_mlp(mesh.shape["g"], out_heads, hidden, gain_mlp[None, :], w_o, w_gate, w_up, w_down)
        return out_hidden, new_lat, new_rope

    return jax.shard_map(local_step, mesh=mesh, in_specs=in_specs, out_specs=(row_spec, row_spec, row_spec), check_vma=False)
```

```python
import functools

import jax
import jax.numpy as jnp
import numpy as np
from jax import lax
from jax.experimental import pallas as pl
from jax.experimental.pallas import tpu as pltpu
from jax.sharding import PartitionSpec as P

MESH = pl.DeviceIdType.MESH
HEAD_GRP = 16
DQ_K = 1024


def proj_kernel(n_dev, lens_ref, x_ref, freq_ref, ga_ref, gq_ref, gkv_ref, wdq_hbm, wdkv_hbm, wuq_hbm, wqr_hbm, wuk_hbm,
                q_out, q2_out, nl_out, nr_out,
                wdq, wdkv, wuq, wqr, wuk, a_all, t_all, c_all, ang, kv_buf, kv_send, qh, qx, rh, rx,
                w_sem, x_sem, q_sem):
    rows, d_model = x_ref.shape
    f32, bf16 = jnp.float32, jnp.bfloat16
    nt = (((1,), (1,)), ((), ()))
    pair = 2 * rows
    q_half = wdq.shape[1]
    q_dim = 2 * q_half
    kv_dim = gkv_ref.shape[0] * 128
    kv_cols = wdkv.shape[0]
    kv_lo = kv_dim // 2
    n_grp = wuq.shape[0]
    my_heads = n_grp * HEAD_GRP
    n_dim = wuq.shape[3]
    me = lax.axis_index("g")
    core = me % 2
    peer = me + 1 - 2 * core
    my_rows = pl.ds(pl.multiple_of(core * rows, rows), rows)
    peer_rows = pl.ds(pl.multiple_of((1 - core) * rows, rows), rows)
    n_dq = d_model // DQ_K
    loads = []
    for k in range(n_dq):
        loads.append(pltpu.make_async_copy(wdq_hbm.at[pl.ds(k * DQ_K, DQ_K), pl.ds(pl.multiple_of(core * q_half, q_half), q_half)], wdq.at[pl.ds(k * DQ_K, DQ_K)], w_sem.at[k]))
    dkv_load = pltpu.make_async_copy(wdkv_hbm.at[pl.ds(pl.multiple_of(core * kv_lo, kv_lo), kv_cols)], wdkv, w_sem.at[n_dq])
    loads.append(dkv_load)
    uq_loads, uk_loads = [], []
    for g in range(n_grp):
        heads = pl.ds(pl.multiple_of(core * my_heads + g * HEAD_GRP, HEAD_GRP), HEAD_GRP)
        uq_loads.append(pltpu.make_async_copy(wuq_hbm.at[:, heads], wuq.at[g], w_sem.at[n_dq + 1 + g]))
        uk_loads.append(pltpu.make_async_copy(wuk_hbm.at[:, heads], wuk.at[g], w_sem.at[n_dq + 1 + n_grp + g]))
        loads += [uq_loads[g], uk_loads[g]]
    qr_rows = wqr.shape[0]
    qr_load = pltpu.make_async_copy(wqr_hbm.at[pl.ds(pl.multiple_of(core * qr_rows, qr_rows), qr_rows)], wqr, w_sem.at[n_dq + 1 + 2 * n_grp])
    loads.append(qr_load)
    for cp in loads:
        cp.start()

    def remote(src, dst, i):
        return pltpu.make_async_remote_copy(src_ref=src, dst_ref=dst, send_sem=x_sem.at[0, i], recv_sem=x_sem.at[1, i], device_id={"g": peer}, device_id_type=MESH)

    row_id = lax.broadcasted_iota(jnp.int32, (rows, 128), 0)
    pos = jnp.zeros((rows, 128), jnp.int32)
    for r in range(rows):
        pos = jnp.where(row_id == r, lens_ref[r], pos)
    ang[my_rows, :] = pos.astype(f32) * freq_ref[...]
    lanes = jnp.zeros((rows, 128), f32)
    for c in range(0, d_model, 512):
        v = x_ref[:, c : c + 512].astype(f32)
        sq = v * v
        lanes = lanes + ((sq[:, :128] + sq[:, 128:256]) + (sq[:, 256:384] + sq[:, 384:]))
    inv = lax.rsqrt(jnp.sum(lanes, axis=1, keepdims=True) / d_model + 1e-6)
    ga_rows = ga_ref[...].astype(f32)
    for c in range(0, d_model, 128):
        v = x_ref[:, c : c + 128].astype(f32)
        a_all[my_rows, c : c + 128] = (v * inv * ga_rows[c // 128 : c // 128 + 1]).astype(bf16)
    barrier = pltpu.get_barrier_semaphore()
    pl.semaphore_signal(barrier, inc=1, device_id={"g": peer}, device_id_type=MESH)
    pl.semaphore_wait(barrier, 1)
    a_copy = remote(a_all.at[my_rows], a_all.at[my_rows], 0)
    ang_copy = remote(ang.at[my_rows], ang.at[my_rows], 1)
    a_copy.start()
    ang_copy.start()
    a_copy.wait()
    ang_copy.wait()

    t = jnp.zeros((pair, q_half), f32)
    for k in range(n_dq):
        loads[k].wait()
        t = t + jnp.dot(a_all[:, k * DQ_K : (k + 1) * DQ_K], wdq[k * DQ_K : (k + 1) * DQ_K], preferred_element_type=f32)
    t_all[core] = t
    t_copy = remote(t_all.at[core], t_all.at[core], 2)
    t_copy.start()

    dkv_load.wait()
    kv_send[:, :kv_cols] = lax.dot_general(a_all[...], wdkv[...], nt, preferred_element_type=f32)
    kv_send[:, kv_cols:] = jnp.zeros((pair, kv_send.shape[1] - kv_cols), f32)
    kv_copy = remote(kv_send.at[peer_rows], kv_buf.at[core], 3)
    kv_copy.start()
    kv_buf[core] = kv_send[my_rows, :]

    lane = lax.broadcasted_iota(jnp.int32, (1, 128), 1)
    low_half = lane % 64 < 32
    cos_all = jnp.cos(ang[...])
    sin_all = jnp.where(low_half, -jnp.sin(ang[...]), jnp.sin(ang[...]))

    def rope(v, cos_part, sin_part):
        swapped = jnp.where(low_half, pltpu.roll(v, 96, 1), pltpu.roll(v, 32, 1))
        return (v * cos_part + swapped * sin_part).astype(bf16)

    t_copy.wait()
    t0, t1 = t_all[0], t_all[1]
    inv = lax.rsqrt((jnp.sum(t0 * t0, axis=1, keepdims=True) + jnp.sum(t1 * t1, axis=1, keepdims=True)) / q_dim + 1e-6)
    gq_rows = gq_ref[...].astype(f32)
    for c in range(0, q_dim, 128):
        piece = t0[:, c : c + 128] if c < q_half else t1[:, c - q_half : c - q_half + 128]
        c_all[:, c : c + 128] = (piece * inv * gq_rows[c // 128 : c // 128 + 1]).astype(bf16)

    half_grp = HEAD_GRP // 2
    q_copies = []
    for g in range(n_grp):
        uq_loads[g].wait()
        w = wuq[g].reshape(q_dim, HEAD_GRP * n_dim)
        q_nope = jnp.dot(c_all[...], w, preferred_element_type=f32).astype(bf16)
        uk_loads[g].wait()
        w = wuk[g].reshape(kv_dim, HEAD_GRP * n_dim)
        for hh in range(HEAD_GRP):
            at = (hh % 2) * (my_heads // 2) + g * half_grp + hh // 2
            span = slice(hh * n_dim, (hh + 1) * n_dim)
            qh[at] = lax.dot_general(q_nope[:, span], w[:, span], nt, preferred_element_type=f32).astype(bf16)
        for odd in range(2):
            at = pl.ds(odd * (my_heads // 2) + g * half_grp, half_grp)
            i = 2 * g + odd
            cp = pltpu.make_async_remote_copy(src_ref=qh.at[at, peer_rows], dst_ref=qx.at[at], send_sem=q_sem.at[0, i], recv_sem=q_sem.at[1, i], device_id={"g": peer}, device_id_type=MESH)
            cp.start()
            q_copies.append(cp)

    qr_load.wait()
    blk = 512
    for b in range(qr_rows // blk):
        v = lax.dot_general(c_all[...], wqr[b * blk : (b + 1) * blk], nt, preferred_element_type=f32)
        for p in range(blk // 128):
            rh[b * (blk // 128) + p] = rope(v[:, p * 128 : (p + 1) * 128], cos_all, sin_all)
    r_copy = remote(rh.at[:, peer_rows], rx, 4)
    r_copy.start()

    kv_copy.wait()
    k0, k1 = kv_buf[0], kv_buf[1]
    lo, hi = k0[:, :kv_lo], k1[:, :kv_lo]
    inv = lax.rsqrt((jnp.sum(lo * lo, axis=1, keepdims=True) + jnp.sum(hi * hi, axis=1, keepdims=True)) / kv_dim + 1e-6)
    gkv_rows = gkv_ref[...].astype(f32)
    for c in range(0, kv_dim, 128):
        piece = lo[:, c : c + 128] if c < kv_lo else hi[:, c - kv_lo : c - kv_lo + 128]
        nl_out[:, c : c + 128] = (piece * inv * gkv_rows[c // 128 : c // 128 + 1]).astype(bf16)
    ang_mine = ang[my_rows, :]
    nr = rope(k1[:, kv_lo : kv_lo + 128], jnp.cos(ang_mine), jnp.where(low_half, -jnp.sin(ang_mine), jnp.sin(ang_mine)))
    nr_out[...] = nr[:, : nr_out.shape[1]]

    own0 = core * my_heads
    other0 = (1 - core) * my_heads
    for p in range(0, my_heads, 16):
        q_out[:, pl.ds(pl.multiple_of(own0 + p, 16), 16), :] = jnp.swapaxes(qh[p : p + 16, my_rows, :], 0, 1)
    for cp in q_copies:
        cp.wait()
    for p in range(0, my_heads, 16):
        q_out[:, pl.ds(pl.multiple_of(other0 + p, 16), 16), :] = jnp.swapaxes(qx[p : p + 16], 0, 1)
    n_pair = my_heads // 2
    q2_out[:, pl.ds(pl.multiple_of(core * n_pair, n_pair), n_pair), :] = jnp.swapaxes(rh[:, my_rows, :], 0, 1)
    r_copy.wait()
    q2_out[:, pl.ds(pl.multiple_of((1 - core) * n_pair, n_pair), n_pair), :] = jnp.swapaxes(rx[...], 0, 1)


def projections(n_dev, lens, x, gain_attn, w_dq, gain_q, w_uq, w_qr, w_dkv, gain_kv, w_uk):
    rows, d_model = x.shape
    q_dim, n_heads, n_dim = w_uq.shape
    kv_dim = w_uk.shape[0]
    rope_dim = w_qr.shape[2]
    my_heads = n_heads // 2
    n_grp = my_heads // HEAD_GRP
    pair = 2 * rows
    bf16, f32 = jnp.bfloat16, jnp.float32
    half_rope = rope_dim // 2
    kv_cols = kv_dim // 2 + rope_dim
    kv_wide = -(-kv_cols // 128) * 128
    freq = np.tile(np.float32(10000.0) ** (-np.arange(half_rope, dtype=np.float32) / np.float32(half_rope)), 128 // half_rope)[None, :].astype(np.float32)
    vmem = pl.BlockSpec(memory_space=pltpu.VMEM)
    hbm = pl.BlockSpec(memory_space=pl.ANY)
    dma = pltpu.SemaphoreType.DMA
    qr_rows = my_heads * rope_dim
    return pl.pallas_call(
        functools.partial(proj_kernel, n_dev),
        out_shape=(
            jax.ShapeDtypeStruct((rows, n_heads, kv_dim), bf16),
            jax.ShapeDtypeStruct((rows, n_heads // 2, 2 * rope_dim), bf16),
            jax.ShapeDtypeStruct((rows, kv_dim), bf16),
            jax.ShapeDtypeStruct((rows, rope_dim), bf16),
        ),
        in_specs=[pl.BlockSpec(memory_space=pltpu.SMEM), vmem, vmem, vmem, vmem, vmem, hbm, hbm, hbm, hbm, hbm],
        out_specs=(vmem, vmem, vmem, vmem),
        scratch_shapes=[
            pltpu.VMEM((d_model, q_dim // 2), bf16),
            pltpu.VMEM((kv_cols, d_model), bf16),
            pltpu.VMEM((n_grp, q_dim, HEAD_GRP, n_dim), bf16),
            pltpu.VMEM((qr_rows, q_dim), bf16),
            pltpu.VMEM((n_grp, kv_dim, HEAD_GRP, n_dim), bf16),
            pltpu.VMEM((pair, d_model), bf16),
            pltpu.VMEM((2, pair, q_dim // 2), f32),
            pltpu.VMEM((pair, q_dim), bf16),
            pltpu.VMEM((pair, 128), f32),
            pltpu.VMEM((2, rows, kv_wide), f32),
            pltpu.VMEM((pair, kv_wide), f32),
            pltpu.VMEM((my_heads, pair, kv_dim), bf16),
            pltpu.VMEM((my_heads, rows, kv_dim), bf16),
            pltpu.VMEM((my_heads // 2, pair, 128), bf16),
            pltpu.VMEM((my_heads // 2, rows, 128), bf16),
            dma((d_model // DQ_K + 2 + 2 * n_grp,)),
            dma((2, 5)),
            dma((2, 2 * n_grp)),
        ],
        compiler_params=pltpu.CompilerParams(vmem_limit_bytes=67043328, collective_id=0, has_side_effects=True),
        cost_estimate=pl.CostEstimate(flops=5 * 10**9, bytes_accessed=40 * 10**6, transcendentals=0),
        name="projections",
    )(lens, x, freq, gain_attn.reshape(-1, 128), gain_q.reshape(-1, 128), gain_kv.reshape(-1, 128), w_dq, w_dkv.T, w_uq, jnp.transpose(w_qr, (1, 2, 0)).reshape(-1, q_dim), w_uk)


ATT_BLK = 256
ATT_BUF = 8
UV_HEADS = 16


def attn_kernel(lens_ref, q_hbm, q2_hbm, nl_hbm, nr_hbm, lat_hbm, rope_hbm, wuv_hbm, o_ref, nl_out, nr_out,
                lat_buf, rope_buf, mix, wuv, q_all, q2_all, nl_rows, order, fill, lat_sem, rope_sem, in_sem):
    rows, heads, kv_dim = q_all.shape
    cache_len = lat_hbm.shape[1]
    r_dim = nr_out.shape[1]
    scale = (wuv.shape[2] + r_dim) ** -0.5
    max_blk = cache_len // ATT_BLK
    n_pair = heads // 4
    f32 = jnp.float32

    def blocks(row):
        return (lens_ref[row] + ATT_BLK - 1) // ATT_BLK

    start = jnp.int32(0)
    for num in range(1, max_blk + 1):
        fill[num] = start
        for row in range(rows):
            start = start + (blocks(row) == num).astype(jnp.int32)

    def place(row, carry):
        num = blocks(row)
        at = fill[num]
        order[at] = row
        fill[num] = at + 1
        return carry

    lax.fori_loop(0, rows, place, 0)

    def lat_copy(row, blk, slot):
        span = pl.ds(blk * ATT_BLK, ATT_BLK)
        return pltpu.make_async_copy(lat_hbm.at[row, span], lat_buf.at[slot, span], lat_sem.at[slot, blk])

    def rope_copy(row, slot):
        return pltpu.make_async_copy(rope_hbm.at[row], rope_buf.at[slot], rope_sem.at[slot])

    def fetch(i):
        row, slot = order[i], lax.rem(i, ATT_BUF)
        count = blocks(order[i - i % 2 + 1])
        for blk in range(max_blk):
            @pl.when(blk < count)
            def _():
                lat_copy(row, blk, slot).start()
        rope_copy(row, slot).start()

    def land(i):
        row, slot = order[i], lax.rem(i, ATT_BUF)
        count = blocks(order[i - i % 2 + 1])
        for blk in range(max_blk):
            @pl.when(blk < count)
            def _():
                lat_copy(row, blk, slot).wait()
        rope_copy(row, slot).wait()

    small = [pltpu.make_async_copy(src, dst, in_sem.at[i]) for i, (src, dst) in enumerate(((q_hbm, q_all), (q2_hbm, q2_all), (nl_hbm, nl_out), (nr_hbm, nr_out), (wuv_hbm, wuv)))]
    for i in range(2):
        fetch(i)
    for cp in small[:4]:
        cp.start()
    for i in range(2, ATT_BUF - 2):
        fetch(i)
    small[4].start()
    for cp in small[:4]:
        cp.wait()
    nl_rows[...] = nl_out[...].astype(f32)
    own_col = lax.broadcasted_iota(jnp.int32, (heads, rows), 1)
    nt = (((1,), (1,)), ((), ()))

    def scores(row, slot, span):
        lat = lat_buf[slot, :span]
        q_lat = q_all[row]
        q2 = q2_all[row]
        q_rot = jnp.concatenate([q2[a : a + n_pair, b : b + r_dim] for a in (0, n_pair) for b in (0, r_dim)], axis=0)
        s = lax.dot_general(lat, q_lat, nt, preferred_element_type=f32).T
        s = s + jnp.dot(q_rot, rope_buf[slot, :, :span], preferred_element_type=f32)
        own = lax.dot_general(q_lat, nl_out[...], nt, preferred_element_type=f32) + lax.dot_general(q_rot, nr_out[...], nt, preferred_element_type=f32)
        own = jnp.sum(jnp.where(own_col == row, own, 0.0), axis=1, keepdims=True) * scale
        return s * scale, own

    def softmax(s, own, row, span):
        pos = lax.broadcasted_iota(jnp.int32, (heads, span), 1)
        s = jnp.where(pos < lens_ref[row], s, -jnp.inf)
        top = jnp.maximum(jnp.max(s, axis=1, keepdims=True), own)
        e = jnp.exp(s - top)
        own_e = jnp.exp(own - top)
        inv = 1.0 / (jnp.sum(e, axis=1, keepdims=True) + own_e)
        return (e * inv).astype(jnp.bfloat16), (own_e * inv).astype(jnp.bfloat16).astype(f32)

    def mixed(prob, own_p, row, slot, span):
        acc = jnp.dot(prob, lat_buf[slot, :span], preferred_element_type=f32)
        return (acc + own_p * nl_rows[pl.ds(row, 1), :]).astype(jnp.bfloat16)

    def pair_step(i, carry):
        first, second = 2 * i, 2 * i + 1

        @pl.when(second + ATT_BUF - 2 < rows)
        def _():
            fetch(first + ATT_BUF - 2)
            fetch(second + ATT_BUF - 2)

        land(first)
        land(second)
        pair = ((order[first], lax.rem(first, ATT_BUF)), (order[second], lax.rem(second, ATT_BUF)))
        count = blocks(pair[1][0])
        for num in range(1, max_blk + 1):
            @pl.when(count == num)
            def _():
                span = num * ATT_BLK
                raw = [scores(row, slot, span) for row, slot in pair]
                prob = [softmax(s, own, row, span) for (s, own), (row, _) in zip(raw, pair)]
                for (p, own_p), (row, slot) in zip(prob, pair):
                    mix[row] = mixed(p, own_p, row, slot, span)
        return carry

    lax.fori_loop(0, rows // 2, pair_step, 0)
    small[4].wait()
    v_dim = wuv.shape[2]

    def head_group(grp, carry):
        base = pl.multiple_of(grp * (heads // 2), heads // 2)
        lhs = mix[:, pl.ds(base, heads // 2), :].reshape(rows, heads // 2 * kv_dim)
        for part in range(heads // 2 // UV_HEADS):
            rhs = wuv[:, pl.ds(pl.multiple_of(base + part * UV_HEADS, UV_HEADS), UV_HEADS), :].reshape(kv_dim, UV_HEADS * v_dim)
            for h in range(UV_HEADS):
                head = part * UV_HEADS + h
                at = (head % 2) * (heads // 4) + head // 2
                out = jnp.dot(lhs[:, at * kv_dim : (at + 1) * kv_dim], rhs[:, h * v_dim : (h + 1) * v_dim], preferred_element_type=jnp.float32)
                o_ref[:, pl.ds(pl.multiple_of((base + head) * v_dim, v_dim), v_dim)] = out.astype(jnp.bfloat16)
        return carry

    lax.fori_loop(0, 2, head_group, 0)


def attention(lens, q_abs, q_pairs, new_lat, new_rope, cache_lat, rope_t, w_uv):
    rows, heads, kv_dim = q_abs.shape
    cache_len = cache_lat.shape[1]
    rope_dim = new_rope.shape[1]
    v_dim = w_uv.shape[2]
    vmem = pl.BlockSpec(memory_space=pltpu.VMEM)
    hbm = pl.BlockSpec(memory_space=pl.ANY)
    max_blk = cache_len // ATT_BLK
    return pl.pallas_call(
        attn_kernel,
        out_shape=(jax.ShapeDtypeStruct((rows, heads * v_dim), jnp.bfloat16), jax.ShapeDtypeStruct((rows, kv_dim), jnp.bfloat16), jax.ShapeDtypeStruct((rows, rope_dim), jnp.bfloat16)),
        in_specs=[pl.BlockSpec(memory_space=pltpu.SMEM)] + [hbm] * 7,
        out_specs=(vmem, vmem, vmem),
        scratch_shapes=[
            pltpu.VMEM((ATT_BUF, cache_len, kv_dim), jnp.bfloat16),
            pltpu.VMEM((ATT_BUF, rope_dim, cache_len), jnp.bfloat16),
            pltpu.VMEM((rows, heads, kv_dim), jnp.bfloat16),
            pltpu.VMEM((kv_dim, heads, v_dim), jnp.bfloat16),
            pltpu.VMEM((rows, heads, kv_dim), jnp.bfloat16),
            pltpu.VMEM((rows, heads // 2, 2 * rope_dim), jnp.bfloat16),
            pltpu.VMEM((rows, kv_dim), jnp.float32),
            pltpu.SMEM((rows,), jnp.int32),
            pltpu.SMEM((max_blk + 1,), jnp.int32),
            pltpu.SemaphoreType.DMA((ATT_BUF, max_blk)),
            pltpu.SemaphoreType.DMA((ATT_BUF,)),
            pltpu.SemaphoreType.DMA((5,)),
        ],
        compiler_params=pltpu.CompilerParams(vmem_limit_bytes=67043328),
        cost_estimate=pl.CostEstimate(flops=10**10, bytes_accessed=40 * 10**6, transcendentals=0),
        name="attention",
    )(lens, q_abs, q_pairs, new_lat, new_rope, cache_lat, rope_t, w_uv)


RING = 28
TILE_K = 2048
TILE_N = 256
RS_N = 512
GATHER_LAG = 5
DIRECT = 4


def mlp_kernel(n_dev, o_ref, x_ref, gain_ref, wo_hbm, wg_hbm, wu_hbm, wd_hbm, out_ref,
               ring, o_all, x_all, x_send, h_all, m_all, u_own, u_peer, wd_peer, acc, part, own_part, near, far, fin,
               ring_sem, pair_sem, in_sem, gat_send, gat_recv, u_sem, rs_send, rs_recv):
    rows, d_model = x_ref.shape
    heads_dim = o_ref.shape[1]
    half = d_model // 2
    ff = wg_hbm.shape[1]
    chips = n_dev // 2
    pair = 2 * rows
    total = n_dev * rows
    f32 = jnp.float32
    me = lax.axis_index("g")
    core = me % 2
    chip = me // 2
    peer = chip * 2 + (1 - core)
    right_chip = (chip + 1) % chips
    left_chip = (chip + chips - 1) % chips
    far_chip = (chip + 2) % chips
    right = right_chip * 2 + core
    left = left_chip * 2 + core
    across = far_chip * 2 + core
    col0 = pl.multiple_of(core * half, half)
    other0 = pl.multiple_of((1 - core) * half, half)

    def remote(src, dst, send, recv, dev):
        return pltpu.make_async_remote_copy(src_ref=src, dst_ref=dst, send_sem=send, recv_sem=recv, device_id={"g": dev}, device_id_type=MESH)

    wo_k = heads_dim // TILE_K
    wo_j = half // TILE_N
    n_wo = wo_j * wo_k
    gu_k = d_model // TILE_K
    gu_n = ff // TILE_N
    n_gu = gu_n * 2 * gu_k
    wd_n = half // TILE_N
    rs_n = half // RS_N
    rs_t = RS_N // TILE_N
    n_all = n_wo + n_gu + wd_n

    def ring_copy(src, slot, depth):
        return pltpu.make_async_copy(src, ring.at[slot, pl.ds(0, depth)], ring_sem.at[slot])

    def issue(t):
        slot = t % RING

        @pl.when(t < n_wo)
        def _():
            j, k = t // wo_k, t % wo_k
            ring_copy(wo_hbm.at[pl.ds(pl.multiple_of(k * TILE_K, TILE_K), TILE_K), pl.ds(pl.multiple_of(col0 + j * TILE_N, TILE_N), TILE_N)], slot, TILE_K).start()

        for mat, w_hbm in ((0, wg_hbm), (1, wu_hbm)):
            q = t - n_wo

            @pl.when((q >= 0) & (q < n_gu) & ((q // gu_k) % 2 == mat))
            def _():
                n, k = q // (2 * gu_k), q % gu_k
                ring_copy(w_hbm.at[pl.ds(pl.multiple_of(k * TILE_K, TILE_K), TILE_K), pl.ds(pl.multiple_of(n * TILE_N, TILE_N), TILE_N)], slot, TILE_K).start()

        @pl.when((t >= n_wo + n_gu) & (t < n_all))
        def _():
            n = t - n_wo - n_gu
            ring_copy(wd_hbm.at[:, pl.ds(pl.multiple_of(col0 + n * TILE_N, TILE_N), TILE_N)], slot, ff).start()

    def arrive(t, depth):
        slot = t % RING
        ring_copy(wo_hbm.at[pl.ds(0, depth), pl.ds(0, TILE_N)], slot, depth).wait()
        return slot

    my_rows = pl.ds(pl.multiple_of(core * rows, rows), rows)
    o_load = pltpu.make_async_copy(o_ref, o_all.at[my_rows], in_sem.at[0])
    x_load = pltpu.make_async_copy(x_ref.at[:, pl.ds(col0, half)], x_all.at[my_rows], in_sem.at[1])
    x_other = pltpu.make_async_copy(x_ref.at[:, pl.ds(other0, half)], x_send, in_sem.at[2])
    o_load.start()
    x_other.start()
    x_load.start()

    def first(t, carry):
        issue(t)
        return carry

    lax.fori_loop(0, RING, first, 0)

    barrier = pltpu.get_barrier_semaphore()
    for dev in (peer, left, right, across):
        pl.semaphore_signal(barrier, inc=1, device_id={"g": dev}, device_id_type=MESH)
    pl.semaphore_wait(barrier, 4)

    o_copy = remote(o_all.at[my_rows], o_all.at[my_rows], pair_sem.at[0], pair_sem.at[1], peer)
    x_copy = remote(x_send, x_all.at[my_rows], pair_sem.at[2], pair_sem.at[3], peer)
    wd_copy = remote(wd_hbm.at[:, pl.ds(other0, half)], wd_peer, pair_sem.at[4], pair_sem.at[5], peer)
    o_load.wait()
    o_copy.start()
    x_other.wait()
    x_copy.start()
    wd_copy.start()
    x_load.wait()
    o_copy.wait()
    x_copy.wait()

    def rows_of(c, lo, num):
        return pl.ds(pl.multiple_of(c * pair + lo, rows), num)

    n_send = half // TILE_N

    def block_of(s):
        return core * n_send + s

    def near_copy(s, to_right):
        region = h_all.at[block_of(s), rows_of(chip, 0, pair)]
        side = 0 if to_right else 1
        return remote(region, region, gat_send.at[side, s], gat_recv.at[side, s], right if to_right else left)

    def pass_copy(s, to_right):
        src_chip = left_chip if to_right else right_chip
        region = h_all.at[block_of(s), rows_of(src_chip, 0 if to_right else rows, rows)]
        side = 2 if to_right else 3
        return remote(region, region, gat_send.at[side, s], gat_recv.at[side, s], right if to_right else left)

    def far_copy(s):
        region = h_all.at[block_of(s), rows_of(chip, 0, pair)]
        return remote(region, region, gat_send.at[2, s], gat_recv.at[2, s], across)

    def peer_copy(s):
        region = h_all.at[block_of(s)]
        return remote(region, region, gat_send.at[4, s], gat_recv.at[4, s], peer)

    relayed = n_send - DIRECT

    def gather_step(s):
        sent = s - 1

        @pl.when((sent >= 0) & (sent < n_send))
        def _():
            near_copy(sent, True).start()
            near_copy(sent, False).start()

        @pl.when((sent >= relayed) & (sent < n_send))
        def _():
            far_copy(sent).start()

        here = s - GATHER_LAG

        @pl.when((here >= 0) & (here < n_send))
        def _():
            near_copy(here, True).wait_recv()
            near_copy(here, False).wait_recv()

        @pl.when((here >= 0) & (here < relayed))
        def _():
            pass_copy(here, True).start()
            pass_copy(here, False).start()

        done = s - 2 * GATHER_LAG + 1

        @pl.when((done >= 0) & (done < relayed))
        def _():
            pass_copy(done, True).wait_recv()
            pass_copy(done, False).wait_recv()
            peer_copy(done).start()

        @pl.when((here >= relayed) & (here < n_send))
        def _():
            far_copy(here).wait_recv()
            peer_copy(here).start()

    def wo_step(j, carry):
        gather_step(j)
        slots = [arrive(j * wo_k + k, TILE_K) for k in range(wo_k)]
        prod = jnp.zeros((pair, TILE_N), f32)
        for k in range(wo_k):
            prod = prod + jnp.dot(o_all[:, k * TILE_K : (k + 1) * TILE_K], ring[slots[k]], preferred_element_type=f32)
        xs = x_all[:, pl.ds(pl.multiple_of(j * TILE_N, TILE_N), TILE_N)].astype(f32)
        h_all[block_of(j), rows_of(chip, 0, pair), :] = (xs + prod).astype(jnp.bfloat16)
        for k in range(wo_k):
            issue(j * wo_k + k + RING)
        return carry

    lax.fori_loop(0, wo_j, wo_step, 0)

    def drain(s, carry):
        gather_step(s)
        return carry

    lax.fori_loop(wo_j, max(n_send + GATHER_LAG, relayed + 2 * GATHER_LAG - 1), drain, 0)

    def settle(s, carry):
        peer_copy(s).wait()
        for to_right in (True, False):
            near_copy(s, to_right).wait_send()

        @pl.when(s < relayed)
        def _():
            pass_copy(s, True).wait_send()
            pass_copy(s, False).wait_send()

        @pl.when(s >= relayed)
        def _():
            far_copy(s).wait_send()

        return carry

    lax.fori_loop(0, n_send, settle, 0)

    gain_rows = gain_ref[...].astype(f32)

    def norm_rows(b, carry):
        block = pl.ds(pl.multiple_of(b * 16, 16), 16)
        lanes = jnp.zeros((16, 128), f32)
        for c in range(d_model // TILE_N):
            v = h_all[c, block, :].astype(f32)
            sq = v * v
            lanes = lanes + (sq[:, :128] + sq[:, 128:])
        inv = lax.rsqrt(jnp.sum(lanes, axis=1, keepdims=True) / d_model + 1e-6)
        for c in range(0, d_model, 128):
            v = h_all[c // TILE_N, block, c % TILE_N : c % TILE_N + 128].astype(f32)
            m_all[block, c : c + 128] = (v * inv * gain_rows[c // 128 : c // 128 + 1]).astype(jnp.bfloat16)
        return carry

    lax.fori_loop(0, total // 16, norm_rows, 0)

    def u_copy(n):
        span = pl.ds(pl.multiple_of(n * TILE_N, TILE_N), TILE_N)
        return remote(u_own.at[:, span], u_peer.at[:, span], u_sem.at[0, n], u_sem.at[1, n], peer)

    def gu_step(n, carry):
        t0 = n_wo + n * 2 * gu_k
        slots = [arrive(t0 + i, TILE_K) for i in range(2 * gu_k)]
        g = jnp.zeros((total, TILE_N), f32)
        u = jnp.zeros((total, TILE_N), f32)
        for k in range(gu_k):
            g = g + jnp.dot(m_all[:, k * TILE_K : (k + 1) * TILE_K], ring[slots[k]], preferred_element_type=f32)
        for k in range(gu_k):
            u = u + jnp.dot(m_all[:, k * TILE_K : (k + 1) * TILE_K], ring[slots[gu_k + k]], preferred_element_type=f32)
        for i in range(2 * gu_k):
            issue(t0 + i + RING)
        u_own[:, pl.ds(pl.multiple_of(n * TILE_N, TILE_N), TILE_N)] = (jax.nn.silu(g) * u).astype(jnp.bfloat16)
        u_copy(n).start()
        return carry

    lax.fori_loop(0, gu_n, gu_step, 0)
    wd_copy.wait()
    for n in range(gu_n):
        u_copy(n).wait()

    def rs_near(n, to_right):
        side = 0 if to_right else 1
        c = right_chip if to_right else left_chip
        return remote(part.at[n, rows_of(c, 0, pair)], near.at[side, n], rs_send.at[side, n], rs_recv.at[side, n], right if to_right else left)

    def rs_far(n):
        return remote(part.at[n, rows_of(far_chip, 0, pair)], far.at[n], rs_send.at[2, n], rs_recv.at[2, n], across)

    def out_cols(n):
        return pl.ds(pl.multiple_of(col0 + n * RS_N, RS_N), RS_N)

    def rs_out(n):
        return remote(fin.at[n], out_ref.at[:, out_cols(n)], rs_send.at[3, n], rs_recv.at[3, n], peer)

    def down_step(n, carry):
        for i in range(rs_t):
            slot = arrive(n_wo + n_gu + n * rs_t + i, ff)
            cols = pl.ds(pl.multiple_of(n * RS_N + i * TILE_N, TILE_N), TILE_N)
            acc[...] = jnp.dot(u_own[...], ring[slot, :ff], preferred_element_type=f32) + jnp.dot(u_peer[...], wd_peer[:, cols], preferred_element_type=f32)
            part[n, :, i * TILE_N : (i + 1) * TILE_N] = acc[...].astype(jnp.bfloat16)
            own_part[n, :, i * TILE_N : (i + 1) * TILE_N] = acc[rows_of(chip, 0, pair), :]
        rs_far(n).start()
        for to_right in (True, False):
            rs_near(n, to_right).start()
        return carry

    lax.fori_loop(0, rs_n, down_step, 0)

    def final_step(n, carry):
        rs_far(n).wait_recv()
        for to_right in (True, False):
            rs_near(n, to_right).wait_recv()
        def rows_sum(side):
            blk = slice(side * rows, (side + 1) * rows)
            mlp = own_part[n, blk] + near[0, n, blk].astype(f32) + near[1, n, blk].astype(f32) + far[n, blk].astype(f32)
            resid = jnp.concatenate([h_all[block_of(n * rs_t + i), rows_of(chip, side * rows, rows), :] for i in range(rs_t)], axis=1)
            return (resid.astype(f32) + mlp).astype(jnp.bfloat16)

        low = rows_sum(0)
        high = rows_sum(1)
        out_ref[:, out_cols(n)] = jnp.where(core == 0, low, high)
        fin[n] = jnp.where(core == 0, high, low)
        rs_out(n).start()
        return carry

    lax.fori_loop(0, rs_n, final_step, 0)

    def finish(n, carry):
        rs_out(n).wait()
        rs_far(n).wait_send()
        for to_right in (True, False):
            rs_near(n, to_right).wait_send()
        return carry

    lax.fori_loop(0, rs_n, finish, 0)


def out_proj_mlp(n_dev, o, x, gain, w_o, w_gate, w_up, w_down):
    rows, d_model = x.shape
    half = d_model // 2
    ff = w_gate.shape[1]
    pair, total = 2 * rows, n_dev * rows
    bf16, f32 = jnp.bfloat16, jnp.float32
    vmem = pl.BlockSpec(memory_space=pltpu.VMEM)
    hbm = pl.BlockSpec(memory_space=pl.ANY)
    n_send, rs_n = half // TILE_N, half // RS_N
    dma = pltpu.SemaphoreType.DMA
    return pl.pallas_call(
        functools.partial(mlp_kernel, n_dev),
        out_shape=jax.ShapeDtypeStruct((rows, d_model), bf16),
        in_specs=[hbm, hbm, vmem, hbm, hbm, hbm, hbm],
        out_specs=vmem,
        scratch_shapes=[
            pltpu.VMEM((RING, TILE_K, TILE_N), bf16),
            pltpu.VMEM((pair, o.shape[1]), bf16),
            pltpu.VMEM((pair, half), bf16),
            pltpu.VMEM((rows, half), bf16),
            pltpu.VMEM((d_model // TILE_N, total, TILE_N), bf16),
            pltpu.VMEM((total, d_model), bf16),
            pltpu.VMEM((total, ff), bf16),
            pltpu.VMEM((total, ff), bf16),
            pltpu.VMEM((ff, half), bf16),
            pltpu.VMEM((total, TILE_N), f32),
            pltpu.VMEM((rs_n, total, RS_N), bf16),
            pltpu.VMEM((rs_n, pair, RS_N), f32),
            pltpu.VMEM((2, rs_n, pair, RS_N), bf16),
            pltpu.VMEM((rs_n, pair, RS_N), bf16),
            pltpu.VMEM((rs_n, rows, RS_N), bf16),
            dma((RING,)),
            dma((6,)),
            dma((3,)),
            dma((5, n_send)),
            dma((5, n_send)),
            dma((2, ff // TILE_N)),
            dma((4, rs_n)),
            dma((4, rs_n)),
        ],
        compiler_params=pltpu.CompilerParams(vmem_limit_bytes=67043328, collective_id=1, has_side_effects=True),
        cost_estimate=pl.CostEstimate(flops=2 * 10**10, bytes_accessed=116 * 10**6, transcendentals=0),
        name="out_proj_mlp",
    )(o, x, gain, w_o, w_gate, w_up, w_down)


def solution(mesh):
    row_spec = P(("rep", "g"))
    full_spec = P()
    in_specs = (row_spec, row_spec, row_spec, row_spec, full_spec, full_spec, full_spec, full_spec, full_spec, full_spec, full_spec, full_spec, full_spec, full_spec, full_spec, P(None, "g"), P(None, "g"), P("g", None))
    n_dev = mesh.shape["g"]

    def local_step(hidden, cache_lat, cache_rope, seq_lens, gain_attn, w_dq, gain_q, w_uq, w_qr, w_dkv, gain_kv, w_uk, w_uv, w_o, gain_mlp, w_gate, w_up, w_down):
        q_abs, q_pairs, lat, rope = projections(n_dev, seq_lens, hidden, gain_attn, w_dq, gain_q, w_uq, w_qr, w_dkv, gain_kv, w_uk)
        out_heads, new_lat, new_rope = attention(seq_lens, q_abs, q_pairs, lat, rope, cache_lat, jnp.swapaxes(cache_rope, 1, 2), w_uv)
        out_hidden = out_proj_mlp(n_dev, out_heads, hidden, gain_mlp.reshape(-1, 128), w_o, w_gate, w_up, w_down)
        return out_hidden, new_lat, new_rope

    return jax.shard_map(local_step, mesh=mesh, in_specs=in_specs, out_specs=(row_spec, row_spec, row_spec), check_vma=False)
```

```python
import functools

import jax
import jax.numpy as jnp
import numpy as np
from jax import lax
from jax.experimental import pallas as pl
from jax.experimental.pallas import tpu as pltpu
from jax.sharding import PartitionSpec as P

MESH = pl.DeviceIdType.MESH
HEAD_GRP = 16
DQ_K = 1024


def proj_kernel(n_dev, lens_ref, x_hbm, freq_ref, ga_ref, gq_ref, gkv_ref, wdq_hbm, wdkv_hbm, wuq_hbm, wqr_hbm, wuk_hbm,
                q_out, q2_out, nl_out, nr_out,
                x_ref, wdq, wdkv, wuq, wqr, wuk, a_all, t_all, c_all, ang, kv_buf, kv_send, qh, qx, rh, rx,
                w_sem, x_sem, q_sem):
    rows, d_model = x_ref.shape
    f32, bf16 = jnp.float32, jnp.bfloat16
    nt = (((1,), (1,)), ((), ()))
    pair = 2 * rows
    q_half = wdq.shape[1]
    q_dim = 2 * q_half
    kv_dim = gkv_ref.shape[0] * 128
    kv_cols = wdkv.shape[0]
    kv_lo = kv_dim // 2
    n_grp = wuq.shape[0]
    my_heads = n_grp * HEAD_GRP
    n_dim = wuq.shape[3]
    me = lax.axis_index("g")
    core = me % 2
    peer = me + 1 - 2 * core
    my_rows = pl.ds(pl.multiple_of(core * rows, rows), rows)
    peer_rows = pl.ds(pl.multiple_of((1 - core) * rows, rows), rows)
    n_dq = d_model // DQ_K
    loads = []
    for k in range(n_dq):
        loads.append(pltpu.make_async_copy(wdq_hbm.at[pl.ds(k * DQ_K, DQ_K), pl.ds(pl.multiple_of(core * q_half, q_half), q_half)], wdq.at[pl.ds(k * DQ_K, DQ_K)], w_sem.at[k]))
    dkv_load = pltpu.make_async_copy(wdkv_hbm.at[pl.ds(pl.multiple_of(core * kv_lo, kv_lo), kv_cols)], wdkv, w_sem.at[n_dq])
    loads.append(dkv_load)
    uq_loads, uk_loads = [], []
    for g in range(n_grp):
        heads = pl.ds(pl.multiple_of(core * my_heads + g * HEAD_GRP, HEAD_GRP), HEAD_GRP)
        uq_loads.append(pltpu.make_async_copy(wuq_hbm.at[:, heads], wuq.at[g], w_sem.at[n_dq + 1 + g]))
        uk_loads.append(pltpu.make_async_copy(wuk_hbm.at[:, heads], wuk.at[g], w_sem.at[n_dq + 1 + n_grp + g]))
        loads += [uq_loads[g], uk_loads[g]]
    qr_rows = wqr.shape[0]
    qr_load = pltpu.make_async_copy(wqr_hbm.at[pl.ds(pl.multiple_of(core * qr_rows, qr_rows), qr_rows)], wqr, w_sem.at[n_dq + 1 + 2 * n_grp])
    loads.append(qr_load)
    x_load = pltpu.make_async_copy(x_hbm, x_ref, w_sem.at[n_dq + 2 + 2 * n_grp])
    x_load.start()
    for cp in loads:
        cp.start()
    barrier = pltpu.get_barrier_semaphore()
    pl.semaphore_signal(barrier, inc=1, device_id={"g": peer}, device_id_type=MESH)

    def remote(src, dst, i):
        return pltpu.make_async_remote_copy(src_ref=src, dst_ref=dst, send_sem=x_sem.at[0, i], recv_sem=x_sem.at[1, i], device_id={"g": peer}, device_id_type=MESH)

    row_id = lax.broadcasted_iota(jnp.int32, (rows, 128), 0)
    pos = jnp.zeros((rows, 128), jnp.int32)
    for r in range(rows):
        pos = jnp.where(row_id == r, lens_ref[r], pos)
    ang[my_rows, :] = pos.astype(f32) * freq_ref[...]
    x_load.wait()
    lanes = jnp.zeros((rows, 128), f32)
    for c in range(0, d_model, 512):
        v = x_ref[:, c : c + 512].astype(f32)
        sq = v * v
        lanes = lanes + ((sq[:, :128] + sq[:, 128:256]) + (sq[:, 256:384] + sq[:, 384:]))
    inv = lax.rsqrt(jnp.sum(lanes, axis=1, keepdims=True) / d_model + 1e-6)
    ga_rows = ga_ref[...].astype(f32)
    for c in range(0, d_model, 128):
        v = x_ref[:, c : c + 128].astype(f32)
        a_all[my_rows, c : c + 128] = (v * inv * ga_rows[c // 128 : c // 128 + 1]).astype(bf16)
    pl.semaphore_wait(barrier, 1)
    a_copy = remote(a_all.at[my_rows], a_all.at[my_rows], 0)
    ang_copy = remote(ang.at[my_rows], ang.at[my_rows], 1)
    a_copy.start()
    ang_copy.start()
    a_copy.wait()
    ang_copy.wait()

    t = jnp.zeros((pair, q_half), f32)
    for k in range(n_dq):
        loads[k].wait()
        t = t + jnp.dot(a_all[:, k * DQ_K : (k + 1) * DQ_K], wdq[k * DQ_K : (k + 1) * DQ_K], preferred_element_type=f32)
    t_all[core] = t
    t_copy = remote(t_all.at[core], t_all.at[core], 2)
    t_copy.start()

    dkv_load.wait()
    kv_send[:, :kv_cols] = lax.dot_general(a_all[...], wdkv[...], nt, preferred_element_type=f32)
    kv_send[:, kv_cols:] = jnp.zeros((pair, kv_send.shape[1] - kv_cols), f32)
    kv_copy = remote(kv_send.at[peer_rows], kv_buf.at[core], 3)
    kv_copy.start()
    kv_buf[core] = kv_send[my_rows, :]

    lane = lax.broadcasted_iota(jnp.int32, (1, 128), 1)
    low_half = lane % 64 < 32
    cos_all = jnp.cos(ang[...])
    sin_all = jnp.where(low_half, -jnp.sin(ang[...]), jnp.sin(ang[...]))

    def rope(v, cos_part, sin_part):
        swapped = jnp.where(low_half, pltpu.roll(v, 96, 1), pltpu.roll(v, 32, 1))
        return (v * cos_part + swapped * sin_part).astype(bf16)

    t_copy.wait()
    t0, t1 = t_all[0], t_all[1]
    inv = lax.rsqrt((jnp.sum(t0 * t0, axis=1, keepdims=True) + jnp.sum(t1 * t1, axis=1, keepdims=True)) / q_dim + 1e-6)
    gq_rows = gq_ref[...].astype(f32)
    for c in range(0, q_dim, 128):
        piece = t0[:, c : c + 128] if c < q_half else t1[:, c - q_half : c - q_half + 128]
        c_all[:, c : c + 128] = (piece * inv * gq_rows[c // 128 : c // 128 + 1]).astype(bf16)

    half_grp = HEAD_GRP // 2
    q_copies = []
    for g in range(n_grp):
        uq_loads[g].wait()
        w = wuq[g].reshape(q_dim, HEAD_GRP * n_dim)
        q_nope = jnp.dot(c_all[...], w, preferred_element_type=f32).astype(bf16)
        uk_loads[g].wait()
        w = wuk[g].reshape(kv_dim, HEAD_GRP * n_dim)
        for hh in range(HEAD_GRP):
            at = (hh % 2) * (my_heads // 2) + g * half_grp + hh // 2
            span = slice(hh * n_dim, (hh + 1) * n_dim)
            qh[at] = lax.dot_general(q_nope[:, span], w[:, span], nt, preferred_element_type=f32).astype(bf16)
        for odd in range(2):
            at = pl.ds(odd * (my_heads // 2) + g * half_grp, half_grp)
            i = 2 * g + odd
            cp = pltpu.make_async_remote_copy(src_ref=qh.at[at, peer_rows], dst_ref=qx.at[at], send_sem=q_sem.at[0, i], recv_sem=q_sem.at[1, i], device_id={"g": peer}, device_id_type=MESH)
            cp.start()
            q_copies.append(cp)

    qr_load.wait()
    blk = 512
    for b in range(qr_rows // blk):
        v = lax.dot_general(c_all[...], wqr[b * blk : (b + 1) * blk], nt, preferred_element_type=f32)
        for p in range(blk // 128):
            rh[b * (blk // 128) + p] = rope(v[:, p * 128 : (p + 1) * 128], cos_all, sin_all)
    r_copy = remote(rh.at[:, peer_rows], rx, 4)
    r_copy.start()

    kv_copy.wait()
    k0, k1 = kv_buf[0], kv_buf[1]
    lo, hi = k0[:, :kv_lo], k1[:, :kv_lo]
    inv = lax.rsqrt((jnp.sum(lo * lo, axis=1, keepdims=True) + jnp.sum(hi * hi, axis=1, keepdims=True)) / kv_dim + 1e-6)
    gkv_rows = gkv_ref[...].astype(f32)
    for c in range(0, kv_dim, 128):
        piece = lo[:, c : c + 128] if c < kv_lo else hi[:, c - kv_lo : c - kv_lo + 128]
        nl_out[:, c : c + 128] = (piece * inv * gkv_rows[c // 128 : c // 128 + 1]).astype(bf16)
    ang_mine = ang[my_rows, :]
    nr = rope(k1[:, kv_lo : kv_lo + 128], jnp.cos(ang_mine), jnp.where(low_half, -jnp.sin(ang_mine), jnp.sin(ang_mine)))
    nr_out[...] = nr[:, : nr_out.shape[1]]

    own0 = core * my_heads
    other0 = (1 - core) * my_heads
    for p in range(0, my_heads, 16):
        q_out[:, pl.ds(pl.multiple_of(own0 + p, 16), 16), :] = jnp.swapaxes(qh[p : p + 16, my_rows, :], 0, 1)
    for cp in q_copies:
        cp.wait()
    for p in range(0, my_heads, 16):
        q_out[:, pl.ds(pl.multiple_of(other0 + p, 16), 16), :] = jnp.swapaxes(qx[p : p + 16], 0, 1)
    n_pair = my_heads // 2
    q2_out[:, pl.ds(pl.multiple_of(core * n_pair, n_pair), n_pair), :] = jnp.swapaxes(rh[:, my_rows, :], 0, 1)
    r_copy.wait()
    q2_out[:, pl.ds(pl.multiple_of((1 - core) * n_pair, n_pair), n_pair), :] = jnp.swapaxes(rx[...], 0, 1)


def projections(n_dev, lens, x, gain_attn, w_dq, gain_q, w_uq, w_qr, w_dkv, gain_kv, w_uk):
    rows, d_model = x.shape
    q_dim, n_heads, n_dim = w_uq.shape
    kv_dim = w_uk.shape[0]
    rope_dim = w_qr.shape[2]
    my_heads = n_heads // 2
    n_grp = my_heads // HEAD_GRP
    pair = 2 * rows
    bf16, f32 = jnp.bfloat16, jnp.float32
    half_rope = rope_dim // 2
    kv_cols = kv_dim // 2 + rope_dim
    kv_wide = -(-kv_cols // 128) * 128
    freq = np.tile(np.float32(10000.0) ** (-np.arange(half_rope, dtype=np.float32) / np.float32(half_rope)), 128 // half_rope)[None, :].astype(np.float32)
    vmem = pl.BlockSpec(memory_space=pltpu.VMEM)
    hbm = pl.BlockSpec(memory_space=pl.ANY)
    dma = pltpu.SemaphoreType.DMA
    qr_rows = my_heads * rope_dim
    return pl.pallas_call(
        functools.partial(proj_kernel, n_dev),
        out_shape=(
            jax.ShapeDtypeStruct((rows, n_heads, kv_dim), bf16),
            jax.ShapeDtypeStruct((rows, n_heads // 2, 2 * rope_dim), bf16),
            jax.ShapeDtypeStruct((rows, kv_dim), bf16),
            jax.ShapeDtypeStruct((rows, rope_dim), bf16),
        ),
        in_specs=[pl.BlockSpec(memory_space=pltpu.SMEM), hbm, vmem, vmem, vmem, vmem, hbm, hbm, hbm, hbm, hbm],
        out_specs=(vmem, vmem, vmem, vmem),
        scratch_shapes=[
            pltpu.VMEM((rows, d_model), bf16),
            pltpu.VMEM((d_model, q_dim // 2), bf16),
            pltpu.VMEM((kv_cols, d_model), bf16),
            pltpu.VMEM((n_grp, q_dim, HEAD_GRP, n_dim), bf16),
            pltpu.VMEM((qr_rows, q_dim), bf16),
            pltpu.VMEM((n_grp, kv_dim, HEAD_GRP, n_dim), bf16),
            pltpu.VMEM((pair, d_model), bf16),
            pltpu.VMEM((2, pair, q_dim // 2), f32),
            pltpu.VMEM((pair, q_dim), bf16),
            pltpu.VMEM((pair, 128), f32),
            pltpu.VMEM((2, rows, kv_wide), f32),
            pltpu.VMEM((pair, kv_wide), f32),
            pltpu.VMEM((my_heads, pair, kv_dim), bf16),
            pltpu.VMEM((my_heads, rows, kv_dim), bf16),
            pltpu.VMEM((my_heads // 2, pair, 128), bf16),
            pltpu.VMEM((my_heads // 2, rows, 128), bf16),
            dma((d_model // DQ_K + 3 + 2 * n_grp,)),
            dma((2, 5)),
            dma((2, 2 * n_grp)),
        ],
        compiler_params=pltpu.CompilerParams(vmem_limit_bytes=67043328, collective_id=0, has_side_effects=True),
        cost_estimate=pl.CostEstimate(flops=5 * 10**9, bytes_accessed=40 * 10**6, transcendentals=0),
        name="projections",
    )(lens, x, freq, gain_attn.reshape(-1, 128), gain_q.reshape(-1, 128), gain_kv.reshape(-1, 128), w_dq, w_dkv.T, w_uq, jnp.transpose(w_qr, (1, 2, 0)).reshape(-1, q_dim), w_uk)


ATT_BLK = 256
ATT_BUF = 12
ROWS_STEP = 4
UV_HEADS = 16


def attn_kernel(lens_ref, q_hbm, q2_hbm, nl_hbm, nr_hbm, lat_hbm, rope_hbm, wuv_hbm, o_ref, nl_out, nr_out,
                lat_buf, rope_buf, mix, wuv, q_all, q2_all, nl_rows, order, fill, lat_sem, rope_sem, in_sem):
    rows, heads, kv_dim = q_all.shape
    cache_len = lat_hbm.shape[1]
    r_dim = nr_out.shape[1]
    scale = (wuv.shape[2] + r_dim) ** -0.5
    max_blk = cache_len // ATT_BLK
    n_pair = heads // 4
    f32 = jnp.float32

    def blocks(row):
        return (lens_ref[row] + ATT_BLK - 1) // ATT_BLK

    start = jnp.int32(0)
    for num in range(1, max_blk + 1):
        fill[num] = start
        for row in range(rows):
            start = start + (blocks(row) == num).astype(jnp.int32)

    def place(row, carry):
        num = blocks(row)
        at = fill[num]
        order[at] = row
        fill[num] = at + 1
        return carry

    lax.fori_loop(0, rows, place, 0)

    def lat_copy(row, blk, slot):
        span = pl.ds(blk * ATT_BLK, ATT_BLK)
        return pltpu.make_async_copy(lat_hbm.at[row, span], lat_buf.at[slot, span], lat_sem.at[slot, blk])

    def rope_copy(row, slot):
        return pltpu.make_async_copy(rope_hbm.at[row], rope_buf.at[slot], rope_sem.at[slot])

    def fetch(i):
        row, slot = order[i], lax.rem(i, ATT_BUF)
        count = blocks(order[i - i % ROWS_STEP + ROWS_STEP - 1])
        for blk in range(max_blk):
            @pl.when(blk < count)
            def _():
                lat_copy(row, blk, slot).start()
        rope_copy(row, slot).start()

    def land(i):
        row, slot = order[i], lax.rem(i, ATT_BUF)
        count = blocks(order[i - i % ROWS_STEP + ROWS_STEP - 1])
        for blk in range(max_blk):
            @pl.when(blk < count)
            def _():
                lat_copy(row, blk, slot).wait()
        rope_copy(row, slot).wait()

    small = [pltpu.make_async_copy(src, dst, in_sem.at[i]) for i, (src, dst) in enumerate(((q_hbm, q_all), (q2_hbm, q2_all), (nl_hbm, nl_out), (nr_hbm, nr_out), (wuv_hbm, wuv)))]
    for i in range(2):
        fetch(i)
    for cp in small[:4]:
        cp.start()
    for i in range(2, ATT_BUF - ROWS_STEP):
        fetch(i)
    small[4].start()
    for cp in small[:4]:
        cp.wait()
    nl_rows[...] = nl_out[...].astype(f32)
    own_col = lax.broadcasted_iota(jnp.int32, (heads, rows), 1)
    nt = (((1,), (1,)), ((), ()))

    def scores(row, slot, span):
        lat = lat_buf[slot, :span]
        q_lat = q_all[row]
        q2 = q2_all[row]
        q_rot = jnp.concatenate([q2[a : a + n_pair, b : b + r_dim] for a in (0, n_pair) for b in (0, r_dim)], axis=0)
        s = lax.dot_general(lat, q_lat, nt, preferred_element_type=f32).T
        s = s + jnp.dot(q_rot, rope_buf[slot, :, :span], preferred_element_type=f32)
        own = lax.dot_general(q_lat, nl_out[...], nt, preferred_element_type=f32) + lax.dot_general(q_rot, nr_out[...], nt, preferred_element_type=f32)
        own = jnp.sum(jnp.where(own_col == row, own, 0.0), axis=1, keepdims=True) * scale
        return s * scale, own

    def softmax(s, own, row, span):
        pos = lax.broadcasted_iota(jnp.int32, (heads, span), 1)
        s = jnp.where(pos < lens_ref[row], s, -jnp.inf)
        top = jnp.maximum(jnp.max(s, axis=1, keepdims=True), own)
        e = jnp.exp(s - top)
        own_e = jnp.exp(own - top)
        inv = 1.0 / (jnp.sum(e, axis=1, keepdims=True) + own_e)
        return (e * inv).astype(jnp.bfloat16), (own_e * inv).astype(jnp.bfloat16).astype(f32)

    def mixed(prob, own_p, row, slot, span):
        acc = jnp.dot(prob, lat_buf[slot, :span], preferred_element_type=f32)
        return (acc + own_p * nl_rows[pl.ds(row, 1), :]).astype(jnp.bfloat16)

    def pair_step(i, carry):
        first = ROWS_STEP * i

        @pl.when(first + ATT_BUF < rows + ROWS_STEP)
        def _():
            for r in range(ROWS_STEP):
                fetch(first + ATT_BUF - ROWS_STEP + r)

        for r in range(ROWS_STEP):
            land(first + r)
        pair = [(order[first + r], lax.rem(first + r, ATT_BUF)) for r in range(ROWS_STEP)]
        count = blocks(pair[-1][0])
        for num in range(1, max_blk + 1):
            @pl.when(count == num)
            def _():
                span = num * ATT_BLK
                raw = [scores(row, slot, span) for row, slot in pair]
                prob = [softmax(s, own, row, span) for (s, own), (row, _) in zip(raw, pair)]
                for (p, own_p), (row, slot) in zip(prob, pair):
                    mix[row] = mixed(p, own_p, row, slot, span)
        return carry

    lax.fori_loop(0, rows // ROWS_STEP, pair_step, 0)
    small[4].wait()
    v_dim = wuv.shape[2]

    def head_group(grp, carry):
        base = pl.multiple_of(grp * (heads // 2), heads // 2)
        lhs = mix[:, pl.ds(base, heads // 2), :].reshape(rows, heads // 2 * kv_dim)
        for part in range(heads // 2 // UV_HEADS):
            rhs = wuv[:, pl.ds(pl.multiple_of(base + part * UV_HEADS, UV_HEADS), UV_HEADS), :].reshape(kv_dim, UV_HEADS * v_dim)
            for h in range(UV_HEADS):
                head = part * UV_HEADS + h
                at = (head % 2) * (heads // 4) + head // 2
                out = jnp.dot(lhs[:, at * kv_dim : (at + 1) * kv_dim], rhs[:, h * v_dim : (h + 1) * v_dim], preferred_element_type=jnp.float32)
                o_ref[:, pl.ds(pl.multiple_of((base + head) * v_dim, v_dim), v_dim)] = out.astype(jnp.bfloat16)
        return carry

    lax.fori_loop(0, 2, head_group, 0)


def attention(lens, q_abs, q_pairs, new_lat, new_rope, cache_lat, rope_t, w_uv):
    rows, heads, kv_dim = q_abs.shape
    cache_len = cache_lat.shape[1]
    rope_dim = new_rope.shape[1]
    v_dim = w_uv.shape[2]
    vmem = pl.BlockSpec(memory_space=pltpu.VMEM)
    hbm = pl.BlockSpec(memory_space=pl.ANY)
    max_blk = cache_len // ATT_BLK
    return pl.pallas_call(
        attn_kernel,
        out_shape=(jax.ShapeDtypeStruct((rows, heads * v_dim), jnp.bfloat16), jax.ShapeDtypeStruct((rows, kv_dim), jnp.bfloat16), jax.ShapeDtypeStruct((rows, rope_dim), jnp.bfloat16)),
        in_specs=[pl.BlockSpec(memory_space=pltpu.SMEM)] + [hbm] * 7,
        out_specs=(vmem, vmem, vmem),
        scratch_shapes=[
            pltpu.VMEM((ATT_BUF, cache_len, kv_dim), jnp.bfloat16),
            pltpu.VMEM((ATT_BUF, rope_dim, cache_len), jnp.bfloat16),
            pltpu.VMEM((rows, heads, kv_dim), jnp.bfloat16),
            pltpu.VMEM((kv_dim, heads, v_dim), jnp.bfloat16),
            pltpu.VMEM((rows, heads, kv_dim), jnp.bfloat16),
            pltpu.VMEM((rows, heads // 2, 2 * rope_dim), jnp.bfloat16),
            pltpu.VMEM((rows, kv_dim), jnp.float32),
            pltpu.SMEM((rows,), jnp.int32),
            pltpu.SMEM((max_blk + 1,), jnp.int32),
            pltpu.SemaphoreType.DMA((ATT_BUF, max_blk)),
            pltpu.SemaphoreType.DMA((ATT_BUF,)),
            pltpu.SemaphoreType.DMA((5,)),
        ],
        compiler_params=pltpu.CompilerParams(vmem_limit_bytes=67043328),
        cost_estimate=pl.CostEstimate(flops=10**10, bytes_accessed=40 * 10**6, transcendentals=0),
        name="attention",
    )(lens, q_abs, q_pairs, new_lat, new_rope, cache_lat, rope_t, w_uv)


RING = 28
TILE_K = 2048
TILE_N = 256
RS_N = 256
GATHER_LAG = 5
DIRECT = 2


def mlp_kernel(n_dev, o_ref, x_ref, gain_ref, wo_hbm, wg_hbm, wu_hbm, wd_hbm, out_ref,
               ring, o_all, x_all, x_send, h_all, m_all, u_own, u_peer, wd_peer, acc, part, own_part, near, far, fin,
               ring_sem, pair_sem, in_sem, gat_send, gat_recv, u_sem, rs_send, rs_recv):
    rows, d_model = x_ref.shape
    heads_dim = o_ref.shape[1]
    half = d_model // 2
    ff = wg_hbm.shape[1]
    chips = n_dev // 2
    pair = 2 * rows
    total = n_dev * rows
    f32 = jnp.float32
    me = lax.axis_index("g")
    core = me % 2
    chip = me // 2
    peer = chip * 2 + (1 - core)
    right_chip = (chip + 1) % chips
    left_chip = (chip + chips - 1) % chips
    far_chip = (chip + 2) % chips
    right = right_chip * 2 + core
    left = left_chip * 2 + core
    across = far_chip * 2 + core
    col0 = pl.multiple_of(core * half, half)
    other0 = pl.multiple_of((1 - core) * half, half)

    def remote(src, dst, send, recv, dev):
        return pltpu.make_async_remote_copy(src_ref=src, dst_ref=dst, send_sem=send, recv_sem=recv, device_id={"g": dev}, device_id_type=MESH)

    wo_k = heads_dim // TILE_K
    wo_j = half // TILE_N
    n_wo = wo_j * wo_k
    gu_k = d_model // TILE_K
    gu_n = ff // TILE_N
    n_gu = gu_n * 2 * gu_k
    wd_n = half // TILE_N
    rs_n = half // RS_N
    rs_t = RS_N // TILE_N
    n_all = n_wo + n_gu + wd_n

    def ring_copy(src, slot, depth):
        return pltpu.make_async_copy(src, ring.at[slot, pl.ds(0, depth)], ring_sem.at[slot])

    def issue(t):
        slot = t % RING

        @pl.when(t < n_wo)
        def _():
            j, k = t // wo_k, t % wo_k
            ring_copy(wo_hbm.at[pl.ds(pl.multiple_of(k * TILE_K, TILE_K), TILE_K), pl.ds(pl.multiple_of(col0 + j * TILE_N, TILE_N), TILE_N)], slot, TILE_K).start()

        for mat, w_hbm in ((0, wg_hbm), (1, wu_hbm)):
            q = t - n_wo

            @pl.when((q >= 0) & (q < n_gu) & ((q // gu_k) % 2 == mat))
            def _():
                n, k = q // (2 * gu_k), q % gu_k
                ring_copy(w_hbm.at[pl.ds(pl.multiple_of(k * TILE_K, TILE_K), TILE_K), pl.ds(pl.multiple_of(n * TILE_N, TILE_N), TILE_N)], slot, TILE_K).start()

        @pl.when((t >= n_wo + n_gu) & (t < n_all))
        def _():
            n = t - n_wo - n_gu
            ring_copy(wd_hbm.at[:, pl.ds(pl.multiple_of(col0 + n * TILE_N, TILE_N), TILE_N)], slot, ff).start()

    def arrive(t, depth):
        slot = t % RING
        ring_copy(wo_hbm.at[pl.ds(0, depth), pl.ds(0, TILE_N)], slot, depth).wait()
        return slot

    my_rows = pl.ds(pl.multiple_of(core * rows, rows), rows)
    o_load = pltpu.make_async_copy(o_ref, o_all.at[my_rows], in_sem.at[0])
    x_load = pltpu.make_async_copy(x_ref.at[:, pl.ds(col0, half)], x_all.at[my_rows], in_sem.at[1])
    x_other = pltpu.make_async_copy(x_ref.at[:, pl.ds(other0, half)], x_send, in_sem.at[2])
    o_load.start()
    x_other.start()
    x_load.start()

    barrier = pltpu.get_barrier_semaphore()
    for dev in (peer, left, right, across):
        pl.semaphore_signal(barrier, inc=1, device_id={"g": dev}, device_id_type=MESH)

    def first(t, carry):
        issue(t)
        return carry

    lax.fori_loop(0, RING, first, 0)


    o_copy = remote(o_all.at[my_rows], o_all.at[my_rows], pair_sem.at[0], pair_sem.at[1], peer)
    x_copy = remote(x_send, x_all.at[my_rows], pair_sem.at[2], pair_sem.at[3], peer)
    wd_copy = remote(wd_hbm.at[:, pl.ds(other0, half)], wd_peer, pair_sem.at[4], pair_sem.at[5], peer)
    o_load.wait()
    pl.semaphore_wait(barrier, 4)
    o_copy.start()
    x_other.wait()
    x_copy.start()
    wd_copy.start()
    x_load.wait()
    o_copy.wait()
    x_copy.wait()

    def rows_of(c, lo, num):
        return pl.ds(pl.multiple_of(c * pair + lo, rows), num)

    n_send = half // TILE_N

    def block_of(s):
        return core * n_send + s

    def near_copy(s, to_right):
        region = h_all.at[block_of(s), rows_of(chip, 0, pair)]
        side = 0 if to_right else 1
        return remote(region, region, gat_send.at[side, s], gat_recv.at[side, s], right if to_right else left)

    def pass_copy(s, to_right):
        src_chip = left_chip if to_right else right_chip
        region = h_all.at[block_of(s), rows_of(src_chip, 0 if to_right else rows, rows)]
        side = 2 if to_right else 3
        return remote(region, region, gat_send.at[side, s], gat_recv.at[side, s], right if to_right else left)

    def far_copy(s):
        region = h_all.at[block_of(s), rows_of(chip, 0, pair)]
        return remote(region, region, gat_send.at[2, s], gat_recv.at[2, s], across)

    def peer_copy(s):
        region = h_all.at[block_of(s)]
        return remote(region, region, gat_send.at[4, s], gat_recv.at[4, s], peer)

    relayed = n_send - DIRECT

    def gather_step(s):
        sent = s - 1

        @pl.when((sent >= 0) & (sent < n_send))
        def _():
            near_copy(sent, True).start()
            near_copy(sent, False).start()

        @pl.when((sent >= relayed) & (sent < n_send))
        def _():
            far_copy(sent).start()

        here = s - GATHER_LAG

        @pl.when((here >= 0) & (here < n_send))
        def _():
            near_copy(here, True).wait_recv()
            near_copy(here, False).wait_recv()

        @pl.when((here >= 0) & (here < relayed))
        def _():
            pass_copy(here, True).start()
            pass_copy(here, False).start()

        done = s - 2 * GATHER_LAG + 1

        @pl.when((done >= 0) & (done < relayed))
        def _():
            pass_copy(done, True).wait_recv()
            pass_copy(done, False).wait_recv()
            peer_copy(done).start()

        @pl.when((here >= relayed) & (here < n_send))
        def _():
            far_copy(here).wait_recv()
            peer_copy(here).start()

    def wo_step(j, carry):
        gather_step(j)
        slots = [arrive(j * wo_k + k, TILE_K) for k in range(wo_k)]
        prod = jnp.zeros((pair, TILE_N), f32)
        for k in range(wo_k):
            prod = prod + jnp.dot(o_all[:, k * TILE_K : (k + 1) * TILE_K], ring[slots[k]], preferred_element_type=f32)
        xs = x_all[:, pl.ds(pl.multiple_of(j * TILE_N, TILE_N), TILE_N)].astype(f32)
        h_all[block_of(j), rows_of(chip, 0, pair), :] = (xs + prod).astype(jnp.bfloat16)
        for k in range(wo_k):
            issue(j * wo_k + k + RING)
        return carry

    lax.fori_loop(0, wo_j, wo_step, 0)

    def drain(s, carry):
        gather_step(s)
        return carry

    lax.fori_loop(wo_j, max(n_send + GATHER_LAG, relayed + 2 * GATHER_LAG - 1), drain, 0)

    def settle(s, carry):
        peer_copy(s).wait()
        for to_right in (True, False):
            near_copy(s, to_right).wait_send()

        @pl.when(s < relayed)
        def _():
            pass_copy(s, True).wait_send()
            pass_copy(s, False).wait_send()

        @pl.when(s >= relayed)
        def _():
            far_copy(s).wait_send()

        return carry

    lax.fori_loop(0, n_send, settle, 0)

    gain_rows = gain_ref[...].astype(f32)

    def norm_rows(b, carry):
        block = pl.ds(pl.multiple_of(b * 16, 16), 16)
        lanes = jnp.zeros((16, 128), f32)
        for c in range(d_model // TILE_N):
            v = h_all[c, block, :].astype(f32)
            sq = v * v
            lanes = lanes + (sq[:, :128] + sq[:, 128:])
        inv = lax.rsqrt(jnp.sum(lanes, axis=1, keepdims=True) / d_model + 1e-6)
        for c in range(0, d_model, 128):
            v = h_all[c // TILE_N, block, c % TILE_N : c % TILE_N + 128].astype(f32)
            m_all[block, c : c + 128] = (v * inv * gain_rows[c // 128 : c // 128 + 1]).astype(jnp.bfloat16)
        return carry

    lax.fori_loop(0, total // 16, norm_rows, 0)

    def u_copy(n):
        span = pl.ds(pl.multiple_of(n * TILE_N, TILE_N), TILE_N)
        return remote(u_own.at[:, span], u_peer.at[:, span], u_sem.at[0, n], u_sem.at[1, n], peer)

    def gu_step(n, carry):
        t0 = n_wo + n * 2 * gu_k
        slots = [arrive(t0 + i, TILE_K) for i in range(2 * gu_k)]
        g = jnp.zeros((total, TILE_N), f32)
        u = jnp.zeros((total, TILE_N), f32)
        for k in range(gu_k):
            g = g + jnp.dot(m_all[:, k * TILE_K : (k + 1) * TILE_K], ring[slots[k]], preferred_element_type=f32)
        for k in range(gu_k):
            u = u + jnp.dot(m_all[:, k * TILE_K : (k + 1) * TILE_K], ring[slots[gu_k + k]], preferred_element_type=f32)
        for i in range(2 * gu_k):
            issue(t0 + i + RING)
        u_own[:, pl.ds(pl.multiple_of(n * TILE_N, TILE_N), TILE_N)] = (jax.nn.silu(g) * u).astype(jnp.bfloat16)
        u_copy(n).start()
        return carry

    lax.fori_loop(0, gu_n, gu_step, 0)
    wd_copy.wait()
    for n in range(gu_n):
        u_copy(n).wait()

    def rs_near(n, to_right):
        side = 0 if to_right else 1
        c = right_chip if to_right else left_chip
        return remote(part.at[n, rows_of(c, 0, pair)], near.at[side, n], rs_send.at[side, n], rs_recv.at[side, n], right if to_right else left)

    def rs_far(n):
        return remote(part.at[n, rows_of(far_chip, 0, pair)], far.at[n], rs_send.at[2, n], rs_recv.at[2, n], across)

    def out_cols(n):
        return pl.ds(pl.multiple_of(col0 + n * RS_N, RS_N), RS_N)

    def rs_out(n):
        return remote(fin.at[n], out_ref.at[:, out_cols(n)], rs_send.at[3, n], rs_recv.at[3, n], peer)

    def down_step(n, carry):
        for i in range(rs_t):
            slot = arrive(n_wo + n_gu + n * rs_t + i, ff)
            cols = pl.ds(pl.multiple_of(n * RS_N + i * TILE_N, TILE_N), TILE_N)
            acc[...] = jnp.dot(u_own[...], ring[slot, :ff], preferred_element_type=f32) + jnp.dot(u_peer[...], wd_peer[:, cols], preferred_element_type=f32)
            part[n, :, i * TILE_N : (i + 1) * TILE_N] = acc[...].astype(jnp.bfloat16)
            own_part[n, :, i * TILE_N : (i + 1) * TILE_N] = acc[rows_of(chip, 0, pair), :]
        rs_far(n).start()
        for to_right in (True, False):
            rs_near(n, to_right).start()
        return carry

    lax.fori_loop(0, rs_n, down_step, 0)

    def final_step(n, carry):
        rs_far(n).wait_recv()
        for to_right in (True, False):
            rs_near(n, to_right).wait_recv()
        def rows_sum(side):
            blk = slice(side * rows, (side + 1) * rows)
            mlp = own_part[n, blk] + near[0, n, blk].astype(f32) + near[1, n, blk].astype(f32) + far[n, blk].astype(f32)
            resid = jnp.concatenate([h_all[block_of(n * rs_t + i), rows_of(chip, side * rows, rows), :] for i in range(rs_t)], axis=1)
            return (resid.astype(f32) + mlp).astype(jnp.bfloat16)

        low = rows_sum(0)
        high = rows_sum(1)
        out_ref[:, out_cols(n)] = jnp.where(core == 0, low, high)
        fin[n] = jnp.where(core == 0, high, low)
        rs_out(n).start()
        return carry

    lax.fori_loop(0, rs_n, final_step, 0)

    def finish(n, carry):
        rs_out(n).wait()
        rs_far(n).wait_send()
        for to_right in (True, False):
            rs_near(n, to_right).wait_send()
        return carry

    lax.fori_loop(0, rs_n, finish, 0)


def out_proj_mlp(n_dev, o, x, gain, w_o, w_gate, w_up, w_down):
    rows, d_model = x.shape
    half = d_model // 2
    ff = w_gate.shape[1]
    pair, total = 2 * rows, n_dev * rows
    bf16, f32 = jnp.bfloat16, jnp.float32
    vmem = pl.BlockSpec(memory_space=pltpu.VMEM)
    hbm = pl.BlockSpec(memory_space=pl.ANY)
    n_send, rs_n = half // TILE_N, half // RS_N
    dma = pltpu.SemaphoreType.DMA
    return pl.pallas_call(
        functools.partial(mlp_kernel, n_dev),
        out_shape=jax.ShapeDtypeStruct((rows, d_model), bf16),
        in_specs=[hbm, hbm, vmem, hbm, hbm, hbm, hbm],
        out_specs=vmem,
        scratch_shapes=[
            pltpu.VMEM((RING, TILE_K, TILE_N), bf16),
            pltpu.VMEM((pair, o.shape[1]), bf16),
            pltpu.VMEM((pair, half), bf16),
            pltpu.VMEM((rows, half), bf16),
            pltpu.VMEM((d_model // TILE_N, total, TILE_N), bf16),
            pltpu.VMEM((total, d_model), bf16),
            pltpu.VMEM((total, ff), bf16),
            pltpu.VMEM((total, ff), bf16),
            pltpu.VMEM((ff, half), bf16),
            pltpu.VMEM((total, TILE_N), f32),
            pltpu.VMEM((rs_n, total, RS_N), bf16),
            pltpu.VMEM((rs_n, pair, RS_N), f32),
            pltpu.VMEM((2, rs_n, pair, RS_N), bf16),
            pltpu.VMEM((rs_n, pair, RS_N), bf16),
            pltpu.VMEM((rs_n, rows, RS_N), bf16),
            dma((RING,)),
            dma((6,)),
            dma((3,)),
            dma((5, n_send)),
            dma((5, n_send)),
            dma((2, ff // TILE_N)),
            dma((4, rs_n)),
            dma((4, rs_n)),
        ],
        compiler_params=pltpu.CompilerParams(vmem_limit_bytes=67043328, collective_id=1, has_side_effects=True),
        cost_estimate=pl.CostEstimate(flops=2 * 10**10, bytes_accessed=116 * 10**6, transcendentals=0),
        name="out_proj_mlp",
    )(o, x, gain, w_o, w_gate, w_up, w_down)


def solution(mesh):
    row_spec = P(("rep", "g"))
    full_spec = P()
    in_specs = (row_spec, row_spec, row_spec, row_spec, full_spec, full_spec, full_spec, full_spec, full_spec, full_spec, full_spec, full_spec, full_spec, full_spec, full_spec, P(None, "g"), P(None, "g"), P("g", None))
    n_dev = mesh.shape["g"]

    def local_step(hidden, cache_lat, cache_rope, seq_lens, gain_attn, w_dq, gain_q, w_uq, w_qr, w_dkv, gain_kv, w_uk, w_uv, w_o, gain_mlp, w_gate, w_up, w_down):
        q_abs, q_pairs, lat, rope = projections(n_dev, seq_lens, hidden, gain_attn, w_dq, gain_q, w_uq, w_qr, w_dkv, gain_kv, w_uk)
        out_heads, new_lat, new_rope = attention(seq_lens, q_abs, q_pairs, lat, rope, cache_lat, jnp.swapaxes(cache_rope, 1, 2), w_uv)
        out_hidden = out_proj_mlp(n_dev, out_heads, hidden, gain_mlp.reshape(-1, 128), w_o, w_gate, w_up, w_down)
        return out_hidden, new_lat, new_rope

    return jax.shard_map(local_step, mesh=mesh, in_specs=in_specs, out_specs=(row_spec, row_spec, row_spec), check_vma=False)
```

```python
import functools

import jax
import jax.numpy as jnp
import numpy as np
from jax import lax
from jax.experimental import pallas as pl
from jax.experimental.pallas import tpu as pltpu
from jax.sharding import PartitionSpec as P

MESH = pl.DeviceIdType.MESH
HEAD_GRP = 16
DQ_K = 1024


def proj_kernel(n_dev, lens_ref, x_hbm, freq_ref, ga_ref, gq_ref, gkv_ref, wdq_hbm, wdkv_hbm, wuq_hbm, wqr_hbm, wuk_hbm,
                q_hbm, q2_out, nl_out, nr_out,
                q_out, x_ref, wdq, wdkv, wuq, wqr, wuk, a_all, t_all, c_all, ang, kv_buf, kv_send, qh, qx, rh, rx,
                w_sem, x_sem, q_sem, out_sem):
    rows, d_model = x_ref.shape
    f32, bf16 = jnp.float32, jnp.bfloat16
    nt = (((1,), (1,)), ((), ()))
    pair = 2 * rows
    q_half = wdq.shape[1]
    q_dim = 2 * q_half
    kv_dim = gkv_ref.shape[0] * 128
    kv_cols = wdkv.shape[0]
    kv_lo = kv_dim // 2
    n_grp = wuq.shape[0]
    my_heads = n_grp * HEAD_GRP
    n_dim = wuq.shape[3]
    me = lax.axis_index("g")
    core = me % 2
    peer = me + 1 - 2 * core
    my_rows = pl.ds(pl.multiple_of(core * rows, rows), rows)
    peer_rows = pl.ds(pl.multiple_of((1 - core) * rows, rows), rows)
    n_dq = d_model // DQ_K
    loads = []
    for k in range(n_dq):
        loads.append(pltpu.make_async_copy(wdq_hbm.at[pl.ds(k * DQ_K, DQ_K), pl.ds(pl.multiple_of(core * q_half, q_half), q_half)], wdq.at[pl.ds(k * DQ_K, DQ_K)], w_sem.at[k]))
    dkv_load = pltpu.make_async_copy(wdkv_hbm.at[pl.ds(pl.multiple_of(core * kv_lo, kv_lo), kv_cols)], wdkv, w_sem.at[n_dq])
    loads.append(dkv_load)
    uq_loads, uk_loads = [], []
    for g in range(n_grp):
        heads = pl.ds(pl.multiple_of(core * my_heads + g * HEAD_GRP, HEAD_GRP), HEAD_GRP)
        uq_loads.append(pltpu.make_async_copy(wuq_hbm.at[:, heads], wuq.at[g], w_sem.at[n_dq + 1 + g]))
        uk_loads.append(pltpu.make_async_copy(wuk_hbm.at[:, heads], wuk.at[g], w_sem.at[n_dq + 1 + n_grp + g]))
        loads += [uq_loads[g], uk_loads[g]]
    qr_rows = wqr.shape[0]
    qr_load = pltpu.make_async_copy(wqr_hbm.at[pl.ds(pl.multiple_of(core * qr_rows, qr_rows), qr_rows)], wqr, w_sem.at[n_dq + 1 + 2 * n_grp])
    loads.append(qr_load)
    x_load = pltpu.make_async_copy(x_hbm, x_ref, w_sem.at[n_dq + 2 + 2 * n_grp])
    x_load.start()
    for cp in loads:
        cp.start()
    barrier = pltpu.get_barrier_semaphore()
    pl.semaphore_signal(barrier, inc=1, device_id={"g": peer}, device_id_type=MESH)

    def remote(src, dst, i):
        return pltpu.make_async_remote_copy(src_ref=src, dst_ref=dst, send_sem=x_sem.at[0, i], recv_sem=x_sem.at[1, i], device_id={"g": peer}, device_id_type=MESH)

    row_id = lax.broadcasted_iota(jnp.int32, (rows, 128), 0)
    pos = jnp.zeros((rows, 128), jnp.int32)
    for r in range(rows):
        pos = jnp.where(row_id == r, lens_ref[r], pos)
    ang[my_rows, :] = pos.astype(f32) * freq_ref[...]
    x_load.wait()
    lanes = jnp.zeros((rows, 128), f32)
    for c in range(0, d_model, 512):
        v = x_ref[:, c : c + 512].astype(f32)
        sq = v * v
        lanes = lanes + ((sq[:, :128] + sq[:, 128:256]) + (sq[:, 256:384] + sq[:, 384:]))
    inv = lax.rsqrt(jnp.sum(lanes, axis=1, keepdims=True) / d_model + 1e-6)
    ga_rows = ga_ref[...].astype(f32)
    for c in range(0, d_model, 128):
        v = x_ref[:, c : c + 128].astype(f32)
        a_all[my_rows, c : c + 128] = (v * inv * ga_rows[c // 128 : c // 128 + 1]).astype(bf16)
    pl.semaphore_wait(barrier, 1)
    a_copy = remote(a_all.at[my_rows], a_all.at[my_rows], 0)
    ang_copy = remote(ang.at[my_rows], ang.at[my_rows], 1)
    a_copy.start()
    ang_copy.start()
    a_copy.wait()
    ang_copy.wait()

    t = jnp.zeros((pair, q_half), f32)
    for k in range(n_dq):
        loads[k].wait()
        t = t + jnp.dot(a_all[:, k * DQ_K : (k + 1) * DQ_K], wdq[k * DQ_K : (k + 1) * DQ_K], preferred_element_type=f32)
    t_all[core] = t
    t_copy = remote(t_all.at[core], t_all.at[core], 2)
    t_copy.start()

    dkv_load.wait()
    kv_send[:, :kv_cols] = lax.dot_general(a_all[...], wdkv[...], nt, preferred_element_type=f32)
    kv_send[:, kv_cols:] = jnp.zeros((pair, kv_send.shape[1] - kv_cols), f32)
    kv_copy = remote(kv_send.at[peer_rows], kv_buf.at[core], 3)
    kv_copy.start()
    kv_buf[core] = kv_send[my_rows, :]

    lane = lax.broadcasted_iota(jnp.int32, (1, 128), 1)
    low_half = lane % 64 < 32
    cos_all = jnp.cos(ang[...])
    sin_all = jnp.where(low_half, -jnp.sin(ang[...]), jnp.sin(ang[...]))

    def rope(v, cos_part, sin_part):
        swapped = jnp.where(low_half, pltpu.roll(v, 96, 1), pltpu.roll(v, 32, 1))
        return (v * cos_part + swapped * sin_part).astype(bf16)

    t_copy.wait()
    t0, t1 = t_all[0], t_all[1]
    inv = lax.rsqrt((jnp.sum(t0 * t0, axis=1, keepdims=True) + jnp.sum(t1 * t1, axis=1, keepdims=True)) / q_dim + 1e-6)
    gq_rows = gq_ref[...].astype(f32)
    for c in range(0, q_dim, 128):
        piece = t0[:, c : c + 128] if c < q_half else t1[:, c - q_half : c - q_half + 128]
        c_all[:, c : c + 128] = (piece * inv * gq_rows[c // 128 : c // 128 + 1]).astype(bf16)

    half_grp = HEAD_GRP // 2
    q_copies = []
    for g in range(n_grp):
        uq_loads[g].wait()
        w = wuq[g].reshape(q_dim, HEAD_GRP * n_dim)
        q_nope = jnp.dot(c_all[...], w, preferred_element_type=f32).astype(bf16)
        uk_loads[g].wait()
        w = wuk[g].reshape(kv_dim, HEAD_GRP * n_dim)
        for hh in range(HEAD_GRP):
            at = (hh % 2) * (my_heads // 2) + g * half_grp + hh // 2
            span = slice(hh * n_dim, (hh + 1) * n_dim)
            qh[at] = lax.dot_general(q_nope[:, span], w[:, span], nt, preferred_element_type=f32).astype(bf16)
        for odd in range(2):
            at = pl.ds(odd * (my_heads // 2) + g * half_grp, half_grp)
            i = 2 * g + odd
            cp = pltpu.make_async_remote_copy(src_ref=qh.at[at, peer_rows], dst_ref=qx.at[at], send_sem=q_sem.at[0, i], recv_sem=q_sem.at[1, i], device_id={"g": peer}, device_id_type=MESH)
            cp.start()
            q_copies.append(cp)

    qr_load.wait()
    blk = 512
    for b in range(qr_rows // blk):
        v = lax.dot_general(c_all[...], wqr[b * blk : (b + 1) * blk], nt, preferred_element_type=f32)
        for p in range(blk // 128):
            rh[b * (blk // 128) + p] = rope(v[:, p * 128 : (p + 1) * 128], cos_all, sin_all)
    r_copy = remote(rh.at[:, peer_rows], rx, 4)
    r_copy.start()

    kv_copy.wait()
    k0, k1 = kv_buf[0], kv_buf[1]
    lo, hi = k0[:, :kv_lo], k1[:, :kv_lo]
    inv = lax.rsqrt((jnp.sum(lo * lo, axis=1, keepdims=True) + jnp.sum(hi * hi, axis=1, keepdims=True)) / kv_dim + 1e-6)
    gkv_rows = gkv_ref[...].astype(f32)
    for c in range(0, kv_dim, 128):
        piece = lo[:, c : c + 128] if c < kv_lo else hi[:, c - kv_lo : c - kv_lo + 128]
        nl_out[:, c : c + 128] = (piece * inv * gkv_rows[c // 128 : c // 128 + 1]).astype(bf16)
    ang_mine = ang[my_rows, :]
    nr = rope(k1[:, kv_lo : kv_lo + 128], jnp.cos(ang_mine), jnp.where(low_half, -jnp.sin(ang_mine), jnp.sin(ang_mine)))
    nr_out[...] = nr[:, : nr_out.shape[1]]

    own0 = core * my_heads
    other0 = (1 - core) * my_heads
    for p in range(0, my_heads, 16):
        q_out[:, pl.ds(pl.multiple_of(own0 + p, 16), 16), :] = jnp.swapaxes(qh[p : p + 16, my_rows, :], 0, 1)
    def q_store(first, i):
        at = pl.ds(pl.multiple_of(first, my_heads), my_heads)
        return pltpu.make_async_copy(q_out.at[:, at], q_hbm.at[:, at], out_sem.at[i])

    q_store(own0, 0).start()
    for cp in q_copies:
        cp.wait()
    for p in range(0, my_heads, 16):
        q_out[:, pl.ds(pl.multiple_of(other0 + p, 16), 16), :] = jnp.swapaxes(qx[p : p + 16], 0, 1)
    q_store(other0, 1).start()
    n_pair = my_heads // 2
    q2_out[:, pl.ds(pl.multiple_of(core * n_pair, n_pair), n_pair), :] = jnp.swapaxes(rh[:, my_rows, :], 0, 1)
    r_copy.wait()
    q2_out[:, pl.ds(pl.multiple_of((1 - core) * n_pair, n_pair), n_pair), :] = jnp.swapaxes(rx[...], 0, 1)
    q_store(own0, 0).wait()
    q_store(other0, 1).wait()


def projections(n_dev, lens, x, gain_attn, w_dq, gain_q, w_uq, w_qr, w_dkv, gain_kv, w_uk):
    rows, d_model = x.shape
    q_dim, n_heads, n_dim = w_uq.shape
    kv_dim = w_uk.shape[0]
    rope_dim = w_qr.shape[2]
    my_heads = n_heads // 2
    n_grp = my_heads // HEAD_GRP
    pair = 2 * rows
    bf16, f32 = jnp.bfloat16, jnp.float32
    half_rope = rope_dim // 2
    kv_cols = kv_dim // 2 + rope_dim
    kv_wide = -(-kv_cols // 128) * 128
    freq = np.tile(np.float32(10000.0) ** (-np.arange(half_rope, dtype=np.float32) / np.float32(half_rope)), 128 // half_rope)[None, :].astype(np.float32)
    vmem = pl.BlockSpec(memory_space=pltpu.VMEM)
    hbm = pl.BlockSpec(memory_space=pl.ANY)
    dma = pltpu.SemaphoreType.DMA
    qr_rows = my_heads * rope_dim
    return pl.pallas_call(
        functools.partial(proj_kernel, n_dev),
        out_shape=(
            jax.ShapeDtypeStruct((rows, n_heads, kv_dim), bf16),
            jax.ShapeDtypeStruct((rows, n_heads // 2, 2 * rope_dim), bf16),
            jax.ShapeDtypeStruct((rows, kv_dim), bf16),
            jax.ShapeDtypeStruct((rows, rope_dim), bf16),
        ),
        in_specs=[pl.BlockSpec(memory_space=pltpu.SMEM), hbm, vmem, vmem, vmem, vmem, hbm, hbm, hbm, hbm, hbm],
        out_specs=(hbm, vmem, vmem, vmem),
        scratch_shapes=[
            pltpu.VMEM((rows, n_heads, kv_dim), bf16),
            pltpu.VMEM((rows, d_model), bf16),
            pltpu.VMEM((d_model, q_dim // 2), bf16),
            pltpu.VMEM((kv_cols, d_model), bf16),
            pltpu.VMEM((n_grp, q_dim, HEAD_GRP, n_dim), bf16),
            pltpu.VMEM((qr_rows, q_dim), bf16),
            pltpu.VMEM((n_grp, kv_dim, HEAD_GRP, n_dim), bf16),
            pltpu.VMEM((pair, d_model), bf16),
            pltpu.VMEM((2, pair, q_dim // 2), f32),
            pltpu.VMEM((pair, q_dim), bf16),
            pltpu.VMEM((pair, 128), f32),
            pltpu.VMEM((2, rows, kv_wide), f32),
            pltpu.VMEM((pair, kv_wide), f32),
            pltpu.VMEM((my_heads, pair, kv_dim), bf16),
            pltpu.VMEM((my_heads, rows, kv_dim), bf16),
            pltpu.VMEM((my_heads // 2, pair, 128), bf16),
            pltpu.VMEM((my_heads // 2, rows, 128), bf16),
            dma((d_model // DQ_K + 3 + 2 * n_grp,)),
            dma((2, 5)),
            dma((2, 2 * n_grp)),
            dma((2,)),
        ],
        compiler_params=pltpu.CompilerParams(vmem_limit_bytes=67043328, collective_id=0, has_side_effects=True),
        cost_estimate=pl.CostEstimate(flops=5 * 10**9, bytes_accessed=40 * 10**6, transcendentals=0),
        name="projections",
    )(lens, x, freq, gain_attn.reshape(-1, 128), gain_q.reshape(-1, 128), gain_kv.reshape(-1, 128), w_dq, w_dkv.T, w_uq, jnp.transpose(w_qr, (1, 2, 0)).reshape(-1, q_dim), w_uk)


ATT_BLK = 256
ATT_BUF = 12
ROWS_STEP = 4
UV_HEADS = 16


def attn_kernel(lens_ref, q_hbm, q2_hbm, nl_hbm, nr_hbm, lat_hbm, rope_hbm, wuv_hbm, o_ref, nl_out, nr_out,
                lat_buf, rope_buf, mix, wuv, q_all, q2_all, nl_rows, order, fill, lat_sem, rope_sem, in_sem):
    rows, heads, kv_dim = q_all.shape
    cache_len = lat_hbm.shape[1]
    r_dim = nr_out.shape[1]
    scale = (wuv.shape[2] + r_dim) ** -0.5
    max_blk = cache_len // ATT_BLK
    n_pair = heads // 4
    f32 = jnp.float32

    def blocks(row):
        return (lens_ref[row] + ATT_BLK - 1) // ATT_BLK

    small = [pltpu.make_async_copy(src, dst, in_sem.at[i]) for i, (src, dst) in enumerate(((q_hbm, q_all), (q2_hbm, q2_all), (nl_hbm, nl_out), (nr_hbm, nr_out), (wuv_hbm, wuv)))]
    for cp in small[:4]:
        cp.start()

    start = jnp.int32(0)
    for num in range(1, max_blk + 1):
        fill[num] = start
        for row in range(rows):
            start = start + (blocks(row) == num).astype(jnp.int32)

    def place(row, carry):
        num = blocks(row)
        at = fill[num]
        order[at] = row
        fill[num] = at + 1
        return carry

    lax.fori_loop(0, rows, place, 0)

    def lat_copy(row, blk, slot):
        span = pl.ds(blk * ATT_BLK, ATT_BLK)
        return pltpu.make_async_copy(lat_hbm.at[row, span], lat_buf.at[slot, span], lat_sem.at[slot, blk])

    def rope_copy(row, slot):
        return pltpu.make_async_copy(rope_hbm.at[row], rope_buf.at[slot], rope_sem.at[slot])

    def fetch(i):
        row, slot = order[i], lax.rem(i, ATT_BUF)
        count = blocks(order[i - i % ROWS_STEP + ROWS_STEP - 1])
        for blk in range(max_blk):
            @pl.when(blk < count)
            def _():
                lat_copy(row, blk, slot).start()
        rope_copy(row, slot).start()

    def land(i):
        row, slot = order[i], lax.rem(i, ATT_BUF)
        count = blocks(order[i - i % ROWS_STEP + ROWS_STEP - 1])
        for blk in range(max_blk):
            @pl.when(blk < count)
            def _():
                lat_copy(row, blk, slot).wait()
        rope_copy(row, slot).wait()

    for i in range(2):
        fetch(i)
    for i in range(2, ATT_BUF - ROWS_STEP):
        fetch(i)
    small[4].start()
    for cp in small[:4]:
        cp.wait()
    nl_rows[...] = nl_out[...].astype(f32)
    own_col = lax.broadcasted_iota(jnp.int32, (heads, rows), 1)
    nt = (((1,), (1,)), ((), ()))

    def scores(row, slot, span):
        lat = lat_buf[slot, :span]
        q_lat = q_all[row]
        q2 = q2_all[row]
        q_rot = jnp.concatenate([q2[a : a + n_pair, b : b + r_dim] for a in (0, n_pair) for b in (0, r_dim)], axis=0)
        s = lax.dot_general(lat, q_lat, nt, preferred_element_type=f32).T
        s = s + jnp.dot(q_rot, rope_buf[slot, :, :span], preferred_element_type=f32)
        own = lax.dot_general(q_lat, nl_out[...], nt, preferred_element_type=f32) + lax.dot_general(q_rot, nr_out[...], nt, preferred_element_type=f32)
        own = jnp.sum(jnp.where(own_col == row, own, 0.0), axis=1, keepdims=True) * scale
        return s * scale, own

    def softmax(s, own, row, span):
        pos = lax.broadcasted_iota(jnp.int32, (heads, span), 1)
        s = jnp.where(pos < lens_ref[row], s, -jnp.inf)
        top = jnp.maximum(jnp.max(s, axis=1, keepdims=True), own)
        e = jnp.exp(s - top)
        own_e = jnp.exp(own - top)
        inv = 1.0 / (jnp.sum(e, axis=1, keepdims=True) + own_e)
        return (e * inv).astype(jnp.bfloat16), (own_e * inv).astype(jnp.bfloat16).astype(f32)

    def mixed(prob, own_p, row, slot, span):
        acc = jnp.dot(prob, lat_buf[slot, :span], preferred_element_type=f32)
        return (acc + own_p * nl_rows[pl.ds(row, 1), :]).astype(jnp.bfloat16)

    def pair_step(i, carry):
        first = ROWS_STEP * i

        @pl.when(first + ATT_BUF < rows + ROWS_STEP)
        def _():
            for r in range(ROWS_STEP):
                fetch(first + ATT_BUF - ROWS_STEP + r)

        for r in range(ROWS_STEP):
            land(first + r)
        pair = [(order[first + r], lax.rem(first + r, ATT_BUF)) for r in range(ROWS_STEP)]
        count = blocks(pair[-1][0])
        for num in range(1, max_blk + 1):
            @pl.when(count == num)
            def _():
                span = num * ATT_BLK
                raw = [scores(row, slot, span) for row, slot in pair]
                prob = [softmax(s, own, row, span) for (s, own), (row, _) in zip(raw, pair)]
                for (p, own_p), (row, slot) in zip(prob, pair):
                    mix[row] = mixed(p, own_p, row, slot, span)
        return carry

    lax.fori_loop(0, rows // ROWS_STEP, pair_step, 0)
    small[4].wait()
    v_dim = wuv.shape[2]

    def head_group(grp, carry):
        base = pl.multiple_of(grp * (heads // 2), heads // 2)
        lhs = mix[:, pl.ds(base, heads // 2), :].reshape(rows, heads // 2 * kv_dim)
        for part in range(heads // 2 // UV_HEADS):
            rhs = wuv[:, pl.ds(pl.multiple_of(base + part * UV_HEADS, UV_HEADS), UV_HEADS), :].reshape(kv_dim, UV_HEADS * v_dim)
            for h in range(UV_HEADS):
                head = part * UV_HEADS + h
                at = (head % 2) * (heads // 4) + head // 2
                out = jnp.dot(lhs[:, at * kv_dim : (at + 1) * kv_dim], rhs[:, h * v_dim : (h + 1) * v_dim], preferred_element_type=jnp.float32)
                o_ref[:, pl.ds(pl.multiple_of((base + head) * v_dim, v_dim), v_dim)] = out.astype(jnp.bfloat16)
        return carry

    lax.fori_loop(0, 2, head_group, 0)


def attention(lens, q_abs, q_pairs, new_lat, new_rope, cache_lat, rope_t, w_uv):
    rows, heads, kv_dim = q_abs.shape
    cache_len = cache_lat.shape[1]
    rope_dim = new_rope.shape[1]
    v_dim = w_uv.shape[2]
    vmem = pl.BlockSpec(memory_space=pltpu.VMEM)
    hbm = pl.BlockSpec(memory_space=pl.ANY)
    max_blk = cache_len // ATT_BLK
    return pl.pallas_call(
        attn_kernel,
        out_shape=(jax.ShapeDtypeStruct((rows, heads * v_dim), jnp.bfloat16), jax.ShapeDtypeStruct((rows, kv_dim), jnp.bfloat16), jax.ShapeDtypeStruct((rows, rope_dim), jnp.bfloat16)),
        in_specs=[pl.BlockSpec(memory_space=pltpu.SMEM)] + [hbm] * 7,
        out_specs=(vmem, vmem, vmem),
        scratch_shapes=[
            pltpu.VMEM((ATT_BUF, cache_len, kv_dim), jnp.bfloat16),
            pltpu.VMEM((ATT_BUF, rope_dim, cache_len), jnp.bfloat16),
            pltpu.VMEM((rows, heads, kv_dim), jnp.bfloat16),
            pltpu.VMEM((kv_dim, heads, v_dim), jnp.bfloat16),
            pltpu.VMEM((rows, heads, kv_dim), jnp.bfloat16),
            pltpu.VMEM((rows, heads // 2, 2 * rope_dim), jnp.bfloat16),
            pltpu.VMEM((rows, kv_dim), jnp.float32),
            pltpu.SMEM((rows,), jnp.int32),
            pltpu.SMEM((max_blk + 1,), jnp.int32),
            pltpu.SemaphoreType.DMA((ATT_BUF, max_blk)),
            pltpu.SemaphoreType.DMA((ATT_BUF,)),
            pltpu.SemaphoreType.DMA((5,)),
        ],
        compiler_params=pltpu.CompilerParams(vmem_limit_bytes=67043328),
        cost_estimate=pl.CostEstimate(flops=10**10, bytes_accessed=40 * 10**6, transcendentals=0),
        name="attention",
    )(lens, q_abs, q_pairs, new_lat, new_rope, cache_lat, rope_t, w_uv)


RING = 28
TILE_K = 2048
TILE_N = 256
RS_N = 256
GATHER_LAG = 5
DIRECT = 2


def mlp_kernel(n_dev, o_ref, x_ref, gain_ref, wo_hbm, wg_hbm, wu_hbm, wd_hbm, out_ref,
               ring, o_all, x_all, x_send, h_all, m_all, u_own, u_peer, wd_peer, acc, part, own_part, near, far, fin,
               ring_sem, pair_sem, in_sem, gat_send, gat_recv, u_sem, rs_send, rs_recv):
    rows, d_model = x_ref.shape
    heads_dim = o_ref.shape[1]
    half = d_model // 2
    ff = wg_hbm.shape[1]
    chips = n_dev // 2
    pair = 2 * rows
    total = n_dev * rows
    f32 = jnp.float32
    me = lax.axis_index("g")
    core = me % 2
    chip = me // 2
    peer = chip * 2 + (1 - core)
    right_chip = (chip + 1) % chips
    left_chip = (chip + chips - 1) % chips
    far_chip = (chip + 2) % chips
    right = right_chip * 2 + core
    left = left_chip * 2 + core
    across = far_chip * 2 + core
    col0 = pl.multiple_of(core * half, half)
    other0 = pl.multiple_of((1 - core) * half, half)

    def remote(src, dst, send, recv, dev):
        return pltpu.make_async_remote_copy(src_ref=src, dst_ref=dst, send_sem=send, recv_sem=recv, device_id={"g": dev}, device_id_type=MESH)

    wo_k = heads_dim // TILE_K
    wo_j = half // TILE_N
    n_wo = wo_j * wo_k
    gu_k = d_model // TILE_K
    gu_n = ff // TILE_N
    n_gu = gu_n * 2 * gu_k
    wd_n = half // TILE_N
    rs_n = half // RS_N
    rs_t = RS_N // TILE_N
    n_all = n_wo + n_gu + wd_n

    def ring_copy(src, slot, depth):
        return pltpu.make_async_copy(src, ring.at[slot, pl.ds(0, depth)], ring_sem.at[slot])

    def issue(t):
        slot = t % RING

        @pl.when(t < n_wo)
        def _():
            j, k = t // wo_k, t % wo_k
            ring_copy(wo_hbm.at[pl.ds(pl.multiple_of(k * TILE_K, TILE_K), TILE_K), pl.ds(pl.multiple_of(col0 + j * TILE_N, TILE_N), TILE_N)], slot, TILE_K).start()

        for mat, w_hbm in ((0, wg_hbm), (1, wu_hbm)):
            q = t - n_wo

            @pl.when((q >= 0) & (q < n_gu) & ((q // gu_k) % 2 == mat))
            def _():
                n, k = q // (2 * gu_k), q % gu_k
                ring_copy(w_hbm.at[pl.ds(pl.multiple_of(k * TILE_K, TILE_K), TILE_K), pl.ds(pl.multiple_of(n * TILE_N, TILE_N), TILE_N)], slot, TILE_K).start()

        @pl.when((t >= n_wo + n_gu) & (t < n_all))
        def _():
            n = t - n_wo - n_gu
            ring_copy(wd_hbm.at[:, pl.ds(pl.multiple_of(col0 + n * TILE_N, TILE_N), TILE_N)], slot, ff).start()

    def arrive(t, depth):
        slot = t % RING
        ring_copy(wo_hbm.at[pl.ds(0, depth), pl.ds(0, TILE_N)], slot, depth).wait()
        return slot

    my_rows = pl.ds(pl.multiple_of(core * rows, rows), rows)
    o_load = pltpu.make_async_copy(o_ref, o_all.at[my_rows], in_sem.at[0])
    x_load = pltpu.make_async_copy(x_ref.at[:, pl.ds(col0, half)], x_all.at[my_rows], in_sem.at[1])
    x_other = pltpu.make_async_copy(x_ref.at[:, pl.ds(other0, half)], x_send, in_sem.at[2])
    o_load.start()
    x_other.start()
    x_load.start()

    barrier = pltpu.get_barrier_semaphore()
    for dev in (peer, left, right, across):
        pl.semaphore_signal(barrier, inc=1, device_id={"g": dev}, device_id_type=MESH)

    def first(t, carry):
        issue(t)
        return carry

    lax.fori_loop(0, RING, first, 0)


    o_copy = remote(o_all.at[my_rows], o_all.at[my_rows], pair_sem.at[0], pair_sem.at[1], peer)
    x_copy = remote(x_send, x_all.at[my_rows], pair_sem.at[2], pair_sem.at[3], peer)
    wd_copy = remote(wd_hbm.at[:, pl.ds(other0, half)], wd_peer, pair_sem.at[4], pair_sem.at[5], peer)
    o_load.wait()
    pl.semaphore_wait(barrier, 4)
    o_copy.start()
    x_other.wait()
    x_copy.start()
    wd_copy.start()
    x_load.wait()
    o_copy.wait()
    x_copy.wait()

    def rows_of(c, lo, num):
        return pl.ds(pl.multiple_of(c * pair + lo, rows), num)

    n_send = half // TILE_N

    def block_of(s):
        return core * n_send + s

    def near_copy(s, to_right):
        region = h_all.at[block_of(s), rows_of(chip, 0, pair)]
        side = 0 if to_right else 1
        return remote(region, region, gat_send.at[side, s], gat_recv.at[side, s], right if to_right else left)

    def pass_copy(s, to_right):
        src_chip = left_chip if to_right else right_chip
        region = h_all.at[block_of(s), rows_of(src_chip, 0 if to_right else rows, rows)]
        side = 2 if to_right else 3
        return remote(region, region, gat_send.at[side, s], gat_recv.at[side, s], right if to_right else left)

    def far_copy(s):
        region = h_all.at[block_of(s), rows_of(chip, 0, pair)]
        return remote(region, region, gat_send.at[2, s], gat_recv.at[2, s], across)

    def peer_copy(s):
        region = h_all.at[block_of(s)]
        return remote(region, region, gat_send.at[4, s], gat_recv.at[4, s], peer)

    relayed = n_send - DIRECT

    def gather_step(s):
        sent = s - 1

        @pl.when((sent >= 0) & (sent < n_send))
        def _():
            near_copy(sent, True).start()
            near_copy(sent, False).start()

        @pl.when((sent >= relayed) & (sent < n_send))
        def _():
            far_copy(sent).start()

        here = s - GATHER_LAG

        @pl.when((here >= 0) & (here < n_send))
        def _():
            near_copy(here, True).wait_recv()
            near_copy(here, False).wait_recv()

        @pl.when((here >= 0) & (here < relayed))
        def _():
            pass_copy(here, True).start()
            pass_copy(here, False).start()

        done = s - 2 * GATHER_LAG + 1

        @pl.when((done >= 0) & (done < relayed))
        def _():
            pass_copy(done, True).wait_recv()
            pass_copy(done, False).wait_recv()
            peer_copy(done).start()

        @pl.when((here >= relayed) & (here < n_send))
        def _():
            far_copy(here).wait_recv()
            peer_copy(here).start()

    def wo_step(j, carry):
        gather_step(j)
        slots = [arrive(j * wo_k + k, TILE_K) for k in range(wo_k)]
        prod = jnp.zeros((pair, TILE_N), f32)
        for k in range(wo_k):
            prod = prod + jnp.dot(o_all[:, k * TILE_K : (k + 1) * TILE_K], ring[slots[k]], preferred_element_type=f32)
        xs = x_all[:, pl.ds(pl.multiple_of(j * TILE_N, TILE_N), TILE_N)].astype(f32)
        h_all[block_of(j), rows_of(chip, 0, pair), :] = (xs + prod).astype(jnp.bfloat16)
        for k in range(wo_k):
            issue(j * wo_k + k + RING)
        return carry

    lax.fori_loop(0, wo_j, wo_step, 0)

    def drain(s, carry):
        gather_step(s)
        return carry

    lax.fori_loop(wo_j, max(n_send + GATHER_LAG, relayed + 2 * GATHER_LAG - 1), drain, 0)

    def settle(s, carry):
        peer_copy(s).wait()
        for to_right in (True, False):
            near_copy(s, to_right).wait_send()

        @pl.when(s < relayed)
        def _():
            pass_copy(s, True).wait_send()
            pass_copy(s, False).wait_send()

        @pl.when(s >= relayed)
        def _():
            far_copy(s).wait_send()

        return carry

    lax.fori_loop(0, n_send, settle, 0)

    gain_rows = gain_ref[...].astype(f32)

    def norm_rows(b, carry):
        block = pl.ds(pl.multiple_of(b * 16, 16), 16)
        lanes = jnp.zeros((16, 128), f32)
        for c in range(d_model // TILE_N):
            v = h_all[c, block, :].astype(f32)
            sq = v * v
            lanes = lanes + (sq[:, :128] + sq[:, 128:])
        inv = lax.rsqrt(jnp.sum(lanes, axis=1, keepdims=True) / d_model + 1e-6)
        for c in range(0, d_model, 128):
            v = h_all[c // TILE_N, block, c % TILE_N : c % TILE_N + 128].astype(f32)
            m_all[block, c : c + 128] = (v * inv * gain_rows[c // 128 : c // 128 + 1]).astype(jnp.bfloat16)
        return carry

    lax.fori_loop(0, total // 16, norm_rows, 0)

    def u_copy(n):
        span = pl.ds(pl.multiple_of(n * TILE_N, TILE_N), TILE_N)
        return remote(u_own.at[:, span], u_peer.at[:, span], u_sem.at[0, n], u_sem.at[1, n], peer)

    def gu_step(n, carry):
        t0 = n_wo + n * 2 * gu_k
        slots = [arrive(t0 + i, TILE_K) for i in range(2 * gu_k)]
        g = jnp.zeros((total, TILE_N), f32)
        u = jnp.zeros((total, TILE_N), f32)
        for k in range(gu_k):
            g = g + jnp.dot(m_all[:, k * TILE_K : (k + 1) * TILE_K], ring[slots[k]], preferred_element_type=f32)
        for k in range(gu_k):
            u = u + jnp.dot(m_all[:, k * TILE_K : (k + 1) * TILE_K], ring[slots[gu_k + k]], preferred_element_type=f32)
        for i in range(2 * gu_k):
            issue(t0 + i + RING)
        u_own[:, pl.ds(pl.multiple_of(n * TILE_N, TILE_N), TILE_N)] = (jax.nn.silu(g) * u).astype(jnp.bfloat16)
        u_copy(n).start()
        return carry

    lax.fori_loop(0, gu_n, gu_step, 0)
    wd_copy.wait()
    for n in range(gu_n):
        u_copy(n).wait()

    def rs_near(n, to_right):
        side = 0 if to_right else 1
        c = right_chip if to_right else left_chip
        return remote(part.at[n, rows_of(c, 0, pair)], near.at[side, n], rs_send.at[side, n], rs_recv.at[side, n], right if to_right else left)

    def rs_far(n):
        return remote(part.at[n, rows_of(far_chip, 0, pair)], far.at[n], rs_send.at[2, n], rs_recv.at[2, n], across)

    def out_cols(n):
        return pl.ds(pl.multiple_of(col0 + n * RS_N, RS_N), RS_N)

    def rs_out(n):
        return remote(fin.at[n], out_ref.at[:, out_cols(n)], rs_send.at[3, n], rs_recv.at[3, n], peer)

    def down_step(n, carry):
        for i in range(rs_t):
            slot = arrive(n_wo + n_gu + n * rs_t + i, ff)
            cols = pl.ds(pl.multiple_of(n * RS_N + i * TILE_N, TILE_N), TILE_N)
            acc[...] = jnp.dot(u_own[...], ring[slot, :ff], preferred_element_type=f32) + jnp.dot(u_peer[...], wd_peer[:, cols], preferred_element_type=f32)
            part[n, :, i * TILE_N : (i + 1) * TILE_N] = acc[...].astype(jnp.bfloat16)
            own_part[n, :, i * TILE_N : (i + 1) * TILE_N] = acc[rows_of(chip, 0, pair), :]
        rs_far(n).start()
        for to_right in (True, False):
            rs_near(n, to_right).start()
        return carry

    lax.fori_loop(0, rs_n, down_step, 0)

    def final_step(n, carry):
        rs_far(n).wait_recv()
        for to_right in (True, False):
            rs_near(n, to_right).wait_recv()
        def rows_sum(side):
            blk = slice(side * rows, (side + 1) * rows)
            mlp = own_part[n, blk] + near[0, n, blk].astype(f32) + near[1, n, blk].astype(f32) + far[n, blk].astype(f32)
            resid = jnp.concatenate([h_all[block_of(n * rs_t + i), rows_of(chip, side * rows, rows), :] for i in range(rs_t)], axis=1)
            return (resid.astype(f32) + mlp).astype(jnp.bfloat16)

        low = rows_sum(0)
        high = rows_sum(1)
        out_ref[:, out_cols(n)] = jnp.where(core == 0, low, high)
        fin[n] = jnp.where(core == 0, high, low)
        rs_out(n).start()
        return carry

    lax.fori_loop(0, rs_n, final_step, 0)

    def finish(n, carry):
        rs_out(n).wait()
        rs_far(n).wait_send()
        for to_right in (True, False):
            rs_near(n, to_right).wait_send()
        return carry

    lax.fori_loop(0, rs_n, finish, 0)


def out_proj_mlp(n_dev, o, x, gain, w_o, w_gate, w_up, w_down):
    rows, d_model = x.shape
    half = d_model // 2
    ff = w_gate.shape[1]
    pair, total = 2 * rows, n_dev * rows
    bf16, f32 = jnp.bfloat16, jnp.float32
    vmem = pl.BlockSpec(memory_space=pltpu.VMEM)
    hbm = pl.BlockSpec(memory_space=pl.ANY)
    n_send, rs_n = half // TILE_N, half // RS_N
    dma = pltpu.SemaphoreType.DMA
    return pl.pallas_call(
        functools.partial(mlp_kernel, n_dev),
        out_shape=jax.ShapeDtypeStruct((rows, d_model), bf16),
        in_specs=[hbm, hbm, vmem, hbm, hbm, hbm, hbm],
        out_specs=vmem,
        scratch_shapes=[
            pltpu.VMEM((RING, TILE_K, TILE_N), bf16),
            pltpu.VMEM((pair, o.shape[1]), bf16),
            pltpu.VMEM((pair, half), bf16),
            pltpu.VMEM((rows, half), bf16),
            pltpu.VMEM((d_model // TILE_N, total, TILE_N), bf16),
            pltpu.VMEM((total, d_model), bf16),
            pltpu.VMEM((total, ff), bf16),
            pltpu.VMEM((total, ff), bf16),
            pltpu.VMEM((ff, half), bf16),
            pltpu.VMEM((total, TILE_N), f32),
            pltpu.VMEM((rs_n, total, RS_N), bf16),
            pltpu.VMEM((rs_n, pair, RS_N), f32),
            pltpu.VMEM((2, rs_n, pair, RS_N), bf16),
            pltpu.VMEM((rs_n, pair, RS_N), bf16),
            pltpu.VMEM((rs_n, rows, RS_N), bf16),
            dma((RING,)),
            dma((6,)),
            dma((3,)),
            dma((5, n_send)),
            dma((5, n_send)),
            dma((2, ff // TILE_N)),
            dma((4, rs_n)),
            dma((4, rs_n)),
        ],
        compiler_params=pltpu.CompilerParams(vmem_limit_bytes=67043328, collective_id=1, has_side_effects=True),
        cost_estimate=pl.CostEstimate(flops=2 * 10**10, bytes_accessed=116 * 10**6, transcendentals=0),
        name="out_proj_mlp",
    )(o, x, gain, w_o, w_gate, w_up, w_down)


def solution(mesh):
    row_spec = P(("rep", "g"))
    full_spec = P()
    in_specs = (row_spec, row_spec, row_spec, row_spec, full_spec, full_spec, full_spec, full_spec, full_spec, full_spec, full_spec, full_spec, full_spec, full_spec, full_spec, P(None, "g"), P(None, "g"), P("g", None))
    n_dev = mesh.shape["g"]

    def local_step(hidden, cache_lat, cache_rope, seq_lens, gain_attn, w_dq, gain_q, w_uq, w_qr, w_dkv, gain_kv, w_uk, w_uv, w_o, gain_mlp, w_gate, w_up, w_down):
        q_abs, q_pairs, lat, rope = projections(n_dev, seq_lens, hidden, gain_attn, w_dq, gain_q, w_uq, w_qr, w_dkv, gain_kv, w_uk)
        out_heads, new_lat, new_rope = attention(seq_lens, q_abs, q_pairs, lat, rope, cache_lat, jnp.swapaxes(cache_rope, 1, 2), w_uv)
        out_hidden = out_proj_mlp(n_dev, out_heads, hidden, gain_mlp.reshape(-1, 128), w_o, w_gate, w_up, w_down)
        return out_hidden, new_lat, new_rope

    return jax.shard_map(local_step, mesh=mesh, in_specs=in_specs, out_specs=(row_spec, row_spec, row_spec), check_vma=False)
```
